256 devices in a mesh: view: 8 (over x, core), gauss: 32 (over y, z).
Axes of the slice: x: 4, y: 4, z: 8, core: 2. Of those that a mesh axis runs over, the one named last changes fastest.
Arguments:
- means: float32 [3, 524288], P(None, 'gauss'), may hold values from -1 to 1
- scales: float32 [3, 524288], P(None, 'gauss'), may hold values from 0.05 to 0.6
- quats: float32 [4, 524288], P(None, 'gauss'), may hold values from -6 to 6
- attrs: float32 [49, 524288], P(None, 'gauss'), may hold values from -6 to 6
- grad_screen: float32 [32, 2, 524288], P('view', None, 'gauss'), may hold values from -6 to 6
- visible: int32 [32, 524288], P('view', 'gauss'), may hold values 0 or 1
- clone_mask: int32 [524288], P('gauss'), may hold values from 0 to 1, as said below
- rotation: float32 [32, 3, 3], P('view'), may hold values from -3.5 to 3.5
- shift: float32 [32, 3], P('view'), may hold values from 2 to 5
- focal: float32 [32], P('view'), may hold values from 1 to 4
Outputs:
- peak_stats: float32 [2, 524288], P(None, 'gauss')
- clones: float32 [61, 524288], P(None, 'gauss')
- clone_total: int32 [], replicated
The draws below stay inside these ranges and needn't reach their ends.
Inputs may be any that keep to these rules, and one draw needn't show every extreme that they name: `clone_mask`: in every draw some shard of 16384 consecutive Gaussians has all of them marked.
All inputs are finite; a program needn't handle non-finite values. No bound on the sum of `visible` on one device may be relied on, other than what follows from the above.
Results may differ from the reference program's by a relative error of at most 0.0003.
Values sent between devices are 32-bit elements; how exact they have to be, the bound alone decides.
No kernel may reach another device: no remote copies, remote signals or barrier semaphores. Data moves between devices by JAX's collectives and lax.ppermute only.
A program may use at most 128 MiB of HBM per device.

```python
import math
import jax
import jax.numpy as jnp
from jax import lax

G_DEV = 16384
ATTR = 49
GAUSSIANS = 524288
VIEWS = 32
N_GAUSS = 32


def draw_clone_mask(key, part):
    shards = GAUSSIANS // G_DEV
    most = G_DEV // 128 * 128
    first, second, third = jax.random.split(key, 3)
    raw = jax.random.randint(first, (shards,), 0, most + 1)
    counts = raw * raw // most
    chosen = jax.random.randint(second, (), 0, shards)
    counts = jnp.where(jnp.arange(shards) == chosen, most, counts)
    keys = jax.random.split(third, shards)
    orders = jax.vmap(lambda k: jax.random.permutation(k, G_DEV))(keys)
    return (orders < counts[:, None]).astype(jnp.int32).reshape(-1)


def with_ends(result, stream_key, least, high):
    longest = result.shape.index(max(result.shape))
    spots = []
    for shift in (0, 1):
        where = [jax.random.randint(jax.random.fold_in(stream_key, axis), (), 0, length) for axis, length in enumerate(result.shape)]
        where[longest] = (where[longest] + shift) % result.shape[longest]
        spots.append(tuple(where))
    return result.at[spots[0]].set(least).at[spots[1]].set(high)


def level_of(own_key, extent, pieces, smallest, top_value):
    def one(dim, shards_of):
        steps = jax.random.uniform(jax.random.fold_in(jax.random.fold_in(own_key, 6), dim), (shards_of,), jnp.float32, smallest / len(pieces), top_value / len(pieces))
        return jnp.repeat(jnp.exp(steps), extent[dim] // shards_of).reshape((-1,) + (1,) * (len(extent) - dim - 1))

    loudness = one(*pieces[0])
    for cut in pieces[1:]:
        loudness = loudness * one(*cut)
    return loudness


def centred(own_key, dims, deviation, reach, cuts=(), dtype=jnp.bfloat16):
    result = deviation * jax.random.normal(own_key, dims, jnp.float32)
    if cuts:
        result = result * level_of(own_key, dims, cuts, -0.22, 0.18)
    return jnp.clip(result, -reach, reach).astype(dtype)


def setup_inputs(seed: int = 0) -> dict:
    arg_keys = jax.random.split(jax.random.key(seed), 11)
    return {
        "means": jnp.clip(jax.random.uniform(arg_keys[0], (3, GAUSSIANS), jnp.float32, -1.0, 1.0) * level_of(arg_keys[0], (3, GAUSSIANS), ((1, 32),), -0.4, 0.0), -1.0, 1.0),
        "scales": jnp.clip(jnp.exp(math.log(0.6) - 2.4849067 * jax.random.uniform(arg_keys[1], (3, GAUSSIANS), jnp.float32) ** level_of(arg_keys[1], (3, GAUSSIANS), ((1, 32),), -0.2, 0.2)), 0.05, 0.6),
        "quats": centred(arg_keys[2], (4, GAUSSIANS), 1.0, 6.0, ((1, 32),), jnp.float32),
        "attrs": centred(arg_keys[3], (ATTR, GAUSSIANS), 1.0, 6.0, ((1, 32),), jnp.float32),
        "grad_screen": centred(arg_keys[4], (VIEWS, 2, GAUSSIANS), 1.0, 6.0, ((0, 8), (2, 32)), jnp.float32),
        "visible": with_ends((jax.random.randint(arg_keys[5], (VIEWS, GAUSSIANS), 0, 4) < 3).astype(jnp.int32), jax.random.fold_in(arg_keys[5], 1), 0, 1),
        "clone_mask": draw_clone_mask(jax.random.fold_in(arg_keys[10], 71), 0),
        "rotation": centred(arg_keys[7], (VIEWS, 3, 3), 3 ** -0.5, 3.5, ((0, 8),), jnp.float32),
        "shift": jnp.clip(2.0 + 3.0 * jax.random.uniform(arg_keys[8], (VIEWS, 3), jnp.float32) ** level_of(arg_keys[8], (VIEWS, 3), ((0, 8),), -0.2, 0.2), 2.0, 5.0),
        "focal": jnp.clip(jnp.exp(math.log(4.0) - 1.3862944 * jax.random.uniform(arg_keys[9], (VIEWS,), jnp.float32) ** level_of(arg_keys[9], (VIEWS,), ((0, 8),), -0.2, 0.2)), 1.0, 4.0),
    }


def quat_factor(scales, quats):
    inv = 1.0 / jnp.sqrt(lax.optimization_barrier(jnp.sum(quats * quats, axis=0)) + 0.25)
    w, x, y, z = (quats[0] * inv, quats[1] * inv, quats[2] * inv, quats[3] * inv)
    rq = [[1 - 2 * (y * y + z * z), 2 * (x * y - w * z), 2 * (x * z + w * y)], [2 * (x * y + w * z), 1 - 2 * (x * x + z * z), 2 * (y * z - w * x)], [2 * (x * z - w * y), 2 * (y * z + w * x), 1 - 2 * (x * x + y * y)]]
    return [[rq[i][j] * scales[j] for j in range(3)] for i in range(3)]

def view_stats(means, factor, grad, seen, rot, trans, focal_v):
    point = [rot[i, 0] * means[0] + rot[i, 1] * means[1] + rot[i, 2] * means[2] + trans[i] for i in range(3)]
    depth = jnp.maximum(point[2], 1.0)
    j00 = focal_v / depth
    j02 = -focal_v * point[0] / (depth * depth)
    j12 = -focal_v * point[1] / (depth * depth)
    first = [j00 * rot[0, j] + j02 * rot[2, j] for j in range(3)]
    second = [j00 * rot[1, j] + j12 * rot[2, j] for j in range(3)]
    prow = [sum((first[j] * factor[j][k] for j in range(3))) for k in range(3)]
    qrow = [sum((second[j] * factor[j][k] for j in range(3))) for k in range(3)]
    a_val = prow[0] ** 2 + prow[1] ** 2 + prow[2] ** 2 + 0.3
    c_val = qrow[0] ** 2 + qrow[1] ** 2 + qrow[2] ** 2 + 0.3
    b_val = prow[0] * qrow[0] + prow[1] * qrow[1] + prow[2] * qrow[2]
    half = 0.5 * (a_val - c_val)
    lam = 0.5 * (a_val + c_val) + jnp.sqrt(half * half + b_val * b_val + 0.01)
    seenf = seen.astype(jnp.float32)
    radius = 3.0 * jnp.sqrt(lam) * seenf
    gnorm = jnp.sqrt(grad[0] * grad[0] + grad[1] * grad[1]) * seenf
    return (gnorm, radius)

def reference(means, scales, quats, attrs, grad_screen, visible, clone_mask, rotation, shift, focal):
    factor = quat_factor(scales, quats)
    gmax = jnp.zeros(means.shape[1], jnp.float32)
    rmax = jnp.zeros(means.shape[1], jnp.float32)
    for v in range(grad_screen.shape[0]):
        gnorm, radius = view_stats(means, factor, grad_screen[v], visible[v], rotation[v], shift[v], focal[v])
        gmax = jnp.maximum(gmax, gnorm)
        rmax = jnp.maximum(rmax, radius)
    peak = jnp.stack([gmax, rmax])
    rows = jnp.concatenate([means, scales, quats, attrs, peak], axis=0)
    shards = N_GAUSS
    cap = G_DEV // 128 * 128
    marks = clone_mask.reshape(shards, G_DEV)
    rank = jnp.cumsum(marks, axis=1).astype(jnp.int32) - 1
    counts = lax.optimization_barrier(jnp.sum(marks, axis=1)).astype(jnp.int32)
    blocks = (counts + 127) // 128
    offset = (jnp.cumsum(blocks) - blocks).astype(jnp.int32)
    block = offset[:, None] + rank // 128
    column = block % shards * cap + block // shards * 128 + rank % 128
    column = jnp.where(marks == 1, column, shards * cap).reshape(-1).astype(jnp.int32)
    clones = jnp.zeros((rows.shape[0], shards * cap), jnp.float32).at[:, column].set(rows, mode='drop')
    total = jnp.sum(clone_mask).astype(jnp.int32)
    return (peak, clones, total)
```

```python
import jax
import jax.numpy as jnp
from jax import lax
from jax.experimental import pallas as pl
from jax.experimental.pallas import tpu as pltpu
from jax.sharding import PartitionSpec as P

G_DEV = 16384
LANES = 128
BLOCKS = G_DEV // LANES
SHARDS = 32
PER = BLOCKS // SHARDS
VIEWS_DEV = 4
ROWS = 61
SMEM = pltpu.MemorySpace.SMEM
VMEM = pltpu.MemorySpace.VMEM


def dot(a, b, dims=((1,), (0,))):
    return lax.dot_general(a, b, (dims, ((), ())), preferred_element_type=jnp.float32)


def index_kernel(mask_ref, count_ref, start_ref, index_ref):
    marked = mask_ref[...]
    ones = marked.astype(jnp.float32).astype(jnp.bfloat16)
    row = lax.broadcasted_iota(jnp.int32, (LANES, LANES), 0)
    lane = lax.broadcasted_iota(jnp.int32, (LANES, LANES), 1)
    full = jnp.ones((LANES, LANES), jnp.bfloat16)

    def where_1(cond):
        return jnp.where(cond, 1.0, 0.0).astype(jnp.bfloat16)

    inclusive = dot(ones, where_1(row <= lane)).astype(jnp.int32)
    in_row = dot(ones, full)
    start = dot(where_1(row > lane), in_row.astype(jnp.bfloat16)).astype(jnp.int32)
    in_row_t = dot(jnp.ones((8, LANES), jnp.bfloat16), ones, ((1,), (1,)))
    in_row_tb = in_row_t.astype(jnp.bfloat16)
    start_ref[...] = dot(in_row_tb, where_1(row < lane)).astype(jnp.int32)
    total = dot(in_row_tb, full).astype(jnp.int32)
    for i in range(SHARDS // 8):
        count_ref[8 * i : 8 * i + 8, :] = total

    moves = lane - inclusive + 1
    code = jnp.where(marked == 1, moves * 256 + lane, 0)
    for bit in range(7):
        moved = pltpu.roll(code, LANES - (1 << bit), 1)
        take = ((moved >> (8 + bit)) & 1) == 1
        leave = ((code >> (8 + bit)) & 1) == 1
        code = jnp.where(take, moved, jnp.where(leave, 0, code))
    first = start & (LANES - 1)
    nth = (lane - first) & (LANES - 1)
    source = jnp.take_along_axis(
        code & (LANES - 1), nth, axis=1, mode="promise_in_bounds"
    )
    valid = nth < in_row.astype(jnp.int32)
    here = jnp.where(valid, jnp.where(lane >= first, 256, 512), 0)
    index_ref[...] = source + here


def view_kernel(rot, trans, focal, means, scales, quats, grad, seen, out_ref, scr):
    width = 23

    def group(g, carry):
        for j in range(8):
            col = pl.ds(pl.multiple_of(g * 1024 + j * LANES, LANES), LANES)
            base = j * width
            scr[base : base + 3, :] = means[:, col]
            scr[base + 3 : base + 6, :] = scales[:, col]
            scr[base + 6 : base + 10, :] = quats[:, col]
            for v in range(VIEWS_DEV):
                scr[base + 10 + 2 * v : base + 12 + 2 * v, :] = grad[v, :, col]
            scr[base + 18 : base + 22, :] = seen[:, col].astype(jnp.float32)

        def comp(r):
            return scr[pl.ds(r, 8, stride=width), :]

        m = [comp(i) for i in range(3)]
        sc = [comp(3 + i) for i in range(3)]
        q = [comp(6 + i) for i in range(4)]
        norm = q[0] * q[0] + q[1] * q[1] + q[2] * q[2] + q[3] * q[3]
        inv = 1.0 / jnp.sqrt(norm + 0.25)
        w, x, y, z = (c * inv for c in q)
        rq = [
            [1 - 2 * (y * y + z * z), 2 * (x * y - w * z), 2 * (x * z + w * y)],
            [2 * (x * y + w * z), 1 - 2 * (x * x + z * z), 2 * (y * z - w * x)],
            [2 * (x * z - w * y), 2 * (y * z + w * x), 1 - 2 * (x * x + y * y)],
        ]
        factor = [[rq[i][j] * sc[j] for j in range(3)] for i in range(3)]
        gmax = jnp.zeros((8, LANES), jnp.float32)
        lmax = jnp.zeros((8, LANES), jnp.float32)
        for v in range(VIEWS_DEV):
            r = [[rot[v, 3 * i + j] for j in range(3)] for i in range(3)]
            f = focal[0, v]
            p = [r[i][0] * m[0] + r[i][1] * m[1] + r[i][2] * m[2] + trans[v, i] for i in range(3)]
            over = 1.0 / jnp.maximum(p[2], 1.0)
            j00 = f * over
            j02 = -(j00 * p[0]) * over
            j12 = -(j00 * p[1]) * over
            first = [j00 * r[0][j] + j02 * r[2][j] for j in range(3)]
            second = [j00 * r[1][j] + j12 * r[2][j] for j in range(3)]
            pr = [sum(first[j] * factor[j][k] for j in range(3)) for k in range(3)]
            qr = [sum(second[j] * factor[j][k] for j in range(3)) for k in range(3)]
            a = pr[0] * pr[0] + pr[1] * pr[1] + pr[2] * pr[2] + 0.3
            c = qr[0] * qr[0] + qr[1] * qr[1] + qr[2] * qr[2] + 0.3
            b = pr[0] * qr[0] + pr[1] * qr[1] + pr[2] * qr[2]
            half = 0.5 * (a - c)
            lam = 0.5 * (a + c) + jnp.sqrt(half * half + b * b + 0.01)
            vis = comp(18 + v)
            g0 = comp(10 + 2 * v)
            g1 = comp(11 + 2 * v)
            gmax = jnp.maximum(gmax, (g0 * g0 + g1 * g1) * vis)
            lmax = jnp.maximum(lmax, lam * vis)
        rows = pl.ds(pl.multiple_of(g * 8, 8), 8)
        out_ref[0, rows, :] = gmax
        out_ref[1, rows, :] = lmax
        return carry

    lax.fori_loop(0, G_DEV // 1024, group, 0)


def blocks_before(counts, upto):
    total = jnp.int32(0)
    for t in range(SHARDS):
        total = total + jnp.where(t < upto, (counts[t, 0] + LANES - 1) // LANES, 0)
    return total


def pack_kernel(
    where, counts, start, index, squares, means, scales, quats, low, high, out_ref, peak_ref, rows
):
    view = where[0]
    g_of = lax.broadcasted_iota(jnp.int32, (8, LANES), 0)
    for g in range(BLOCKS // 8):
        norm = jnp.sqrt(squares[0, 8 * g : 8 * g + 8, :])
        radius = 3.0 * jnp.sqrt(squares[1, 8 * g : 8 * g + 8, :])
        for j in range(8):
            col = slice((8 * g + j) * LANES, (8 * g + j + 1) * LANES)
            peak_ref[0:1, col] = norm[j : j + 1, :]
            peak_ref[1:2, col] = radius[j : j + 1, :]

    @pl.when(view == 0)
    def _():
        rows[0:3, :] = means[...]
        rows[3:6, :] = scales[...]
        rows[6:8, :] = quats[0:2, :]

    @pl.when(view == 1)
    def _():
        rows[0:2, :] = quats[2:4, :]

    @pl.when(view > 1)
    def _():
        rows[0:2, :] = low[6:8, :]

    @pl.when((view > 0) & (view < 7))
    def _():
        rows[2:8, :] = high[0:6, :]

    @pl.when(view == 7)
    def _():
        rows[2:3, :] = high[0:1, :]
        rows[3:5, :] = peak_ref[...]
        rows[5:8, :] = jnp.zeros((3, G_DEV), jnp.float32)

    offset = blocks_before(counts, where[1])
    zero = jnp.zeros((8, LANES), jnp.float32)
    for i in range(BLOCKS):
        out_ref[i] = zero

    def place_of(block):
        return ((offset + block) & (SHARDS - 1)) * PER + (block >> 5)

    def eight(i, carry):
        for j in range(8):
            b = i * 8 + j
            block = start[0, b] >> 7
            code = jnp.broadcast_to(index[pl.ds(b, 1), :], (8, LANES))
            tile = rows[:, pl.ds(pl.multiple_of(b * LANES, LANES), LANES)]
            packed = jnp.take_along_axis(
                tile, code & (LANES - 1), axis=1, mode="promise_in_bounds"
            )
            pltpu.store(out_ref.at[place_of(block)], packed, mask=(code & 256) != 0)
            after = jnp.minimum(block + 1, BLOCKS - 1)
            pltpu.store(out_ref.at[place_of(after)], packed, mask=(code & 512) != 0)
        return carry

    lax.fori_loop(0, BLOCKS // 8, eight, 0)


def place_kernel(where, counts, arrived, out_ref, slots):
    cap = out_ref.shape[1]
    mine = where[1]
    zero = jnp.zeros((8, LANES), jnp.float32)
    for i in range(cap):
        slots[i] = zero
    before = jnp.int32(0)
    for s in range(SHARDS):
        local = (mine - before) & (SHARDS - 1)
        first = (before + local) >> 5
        for w in range(PER):
            slots[jnp.minimum(first + w, cap)] = arrived[s * PER + w]
        before = before + (counts[s, 0] + LANES - 1) // LANES
    for i in range(cap):
        tile = slots[i]
        for x in range(4):
            out_ref[x, i] = tile


def join_kernel(where, own, other, out_ref):
    cap = own.shape[1]
    core = where[0] & 1
    mine = pl.ds(pl.multiple_of(8 * core, 8), 8)
    theirs = pl.ds(pl.multiple_of(8 - 8 * core, 8), 8)
    for i in range(BLOCKS):
        col = slice(i * LANES, (i + 1) * LANES)
        if i < cap:
            out_ref[mine, col] = own[0, i]
            out_ref[theirs, col] = other[0, i]
        else:
            out_ref[:, col] = jnp.zeros((16, LANES), jnp.float32)


def smem():
    return pl.BlockSpec(memory_space=SMEM)


def vmem():
    return pl.BlockSpec(memory_space=VMEM)


def body(means, scales, quats, attrs, grad_screen, visible, clone_mask, rotation, shift, focal):
    f32, i32 = jnp.float32, jnp.int32
    view = lax.axis_index("view")
    where = jnp.stack([view, lax.axis_index("gauss")]).astype(i32)

    count, start, index = pl.pallas_call(
        index_kernel,
        in_specs=[vmem()],
        out_specs=[vmem()] * 3,
        out_shape=[
            jax.ShapeDtypeStruct((SHARDS, LANES), i32),
            jax.ShapeDtypeStruct((8, LANES), i32),
            jax.ShapeDtypeStruct((BLOCKS, LANES), i32),
        ],
        name="index",
    )(clone_mask.reshape(BLOCKS, LANES))
    counts = lax.all_to_all(count, "gauss", 0, 0, tiled=True)

    squares = pl.pallas_call(
        view_kernel,
        in_specs=[smem()] * 3 + [vmem()] * 5,
        out_specs=vmem(),
        out_shape=jax.ShapeDtypeStruct((2, BLOCKS, LANES), f32),
        scratch_shapes=[pltpu.VMEM((192, LANES), f32)],
        name="views",
    )(
        rotation.reshape(VIEWS_DEV, 9),
        shift,
        focal.reshape(1, VIEWS_DEV),
        means,
        scales,
        quats,
        grad_screen,
        visible,
    )
    for k in (1, 2, 4):
        pairs = [(v, v ^ k) for v in range(8)]
        squares = jnp.maximum(squares, lax.ppermute(squares, "view", pairs))

    def whole(*shape):
        return pl.BlockSpec(shape, lambda i, w: (0,) * len(shape))

    outgoing, peak = pl.pallas_call(
        pack_kernel,
        grid_spec=pltpu.PrefetchScalarGridSpec(
            num_scalar_prefetch=1,
            grid=(1,),
            in_specs=[
                smem(),
                smem(),
                whole(BLOCKS, LANES),
                whole(2, BLOCKS, LANES),
                whole(3, G_DEV),
                whole(3, G_DEV),
                whole(4, G_DEV),
                pl.BlockSpec((8, G_DEV), lambda i, w: (jnp.maximum(w[0] - 2, 0), 0)),
                pl.BlockSpec((8, G_DEV), lambda i, w: (jnp.maximum(w[0] - 1, 0), 0)),
            ],
            out_specs=[whole(BLOCKS, 8, LANES), whole(2, G_DEV)],
            scratch_shapes=[pltpu.VMEM((8, G_DEV), f32)],
        ),
        out_shape=[
            jax.ShapeDtypeStruct((BLOCKS, 8, LANES), f32),
            jax.ShapeDtypeStruct((2, G_DEV), f32),
        ],
        name="pack",
    )(where, counts, start, index, squares, means, scales, quats, attrs, attrs)

    arrived = lax.all_to_all(
        outgoing.reshape(SHARDS, PER, 8, LANES), "gauss", 0, 0, tiled=True
    ).reshape(BLOCKS, 8, LANES)

    cap = BLOCKS
    piece = pl.pallas_call(
        place_kernel,
        in_specs=[smem(), smem(), vmem()],
        out_specs=vmem(),
        out_shape=jax.ShapeDtypeStruct((4, cap, 8, LANES), f32),
        scratch_shapes=[pltpu.VMEM((cap + 1, 8, LANES), f32)],
        name="place",
    )(where, counts, arrived)
    cores = [[0, 2, 4, 6], [1, 3, 5, 7]]
    own = lax.all_to_all(piece, "view", 0, 0, axis_index_groups=cores, tiled=True)
    other = lax.ppermute(own, "view", [(v, v ^ 1) for v in range(8)])
    clones = pl.pallas_call(
        join_kernel,
        grid_spec=pltpu.PrefetchScalarGridSpec(
            num_scalar_prefetch=1,
            grid=(4,),
            in_specs=[
                pl.BlockSpec((1, cap, 8, LANES), lambda i, w: (i, 0, 0, 0)),
                pl.BlockSpec((1, cap, 8, LANES), lambda i, w: (i, 0, 0, 0)),
            ],
            out_specs=pl.BlockSpec((16, G_DEV), lambda i, w: (i, 0)),
        ),
        out_shape=jax.ShapeDtypeStruct((ROWS, G_DEV), f32),
        name="join",
    )(where, own, other)
    return (peak, clones, jnp.sum(counts[:, 0]))


def solution(mesh):
    return jax.shard_map(
        body,
        mesh=mesh,
        in_specs=(
            P(None, "gauss"),
            P(None, "gauss"),
            P(None, "gauss"),
            P(None, "gauss"),
            P("view", None, "gauss"),
            P("view", "gauss"),
            P("gauss"),
            P("view", None, None),
            P("view", None),
            P("view"),
        ),
        out_specs=(P(None, "gauss"), P(None, "gauss"), P()),
        check_vma=False,
    )
```

```python
import jax
import jax.numpy as jnp
from jax import lax
from jax.experimental import pallas as pl
from jax.experimental.pallas import tpu as pltpu
from jax.sharding import PartitionSpec as P

G_DEV = 16384
LANES = 128
BLOCKS = G_DEV // LANES
SHARDS = 32
PER = BLOCKS // SHARDS
VIEWS_DEV = 4
ROWS = 61
SMEM = pltpu.MemorySpace.SMEM
VMEM = pltpu.MemorySpace.VMEM


def dot(a, b, dims=((1,), (0,))):
    return lax.dot_general(a, b, (dims, ((), ())), preferred_element_type=jnp.float32)


def where_1(cond):
    return jnp.where(cond, 1.0, 0.0).astype(jnp.bfloat16)


def count_kernel(mask_ref, count_ref):
    total = jnp.sum(jnp.sum(mask_ref[...], axis=0, keepdims=True), axis=1, keepdims=True)
    count_ref[...] = jnp.broadcast_to(total, (SHARDS, LANES))


def index_kernel(mask_ref, start_ref, index_ref):
    marked = mask_ref[...]
    ones = marked.astype(jnp.float32).astype(jnp.bfloat16)
    row = lax.broadcasted_iota(jnp.int32, (LANES, LANES), 0)
    lane = lax.broadcasted_iota(jnp.int32, (LANES, LANES), 1)
    full = jnp.ones((LANES, LANES), jnp.bfloat16)

    inclusive = dot(ones, where_1(row <= lane)).astype(jnp.int32)
    in_row = dot(ones, full)
    start = dot(where_1(row > lane), in_row.astype(jnp.bfloat16)).astype(jnp.int32)
    in_row_t = dot(jnp.ones((8, LANES), jnp.bfloat16), ones, ((1,), (1,)))
    start_ref[...] = dot(in_row_t.astype(jnp.bfloat16), where_1(row < lane)).astype(jnp.int32)

    moves = lane - inclusive + 1
    code = jnp.where(marked == 1, moves * 256 + lane, 0)
    for bit in range(7):
        moved = pltpu.roll(code, LANES - (1 << bit), 1)
        take = ((moved >> (8 + bit)) & 1) == 1
        leave = ((code >> (8 + bit)) & 1) == 1
        code = jnp.where(take, moved, jnp.where(leave, 0, code))
    first = start & (LANES - 1)
    nth = (lane - first) & (LANES - 1)
    source = jnp.take_along_axis(
        code & (LANES - 1), nth, axis=1, mode="promise_in_bounds"
    )
    valid = nth < in_row.astype(jnp.int32)
    here = jnp.where(valid, jnp.where(lane >= first, 256, 512), 0)
    index_ref[...] = source + here


def view_kernel(rot, trans, focal, means, scales, quats, grad, seen, out_ref, scr):
    width = 23

    def group(g, carry):
        for j in range(8):
            col = pl.ds(pl.multiple_of(g * 1024 + j * LANES, LANES), LANES)
            base = j * width
            scr[base : base + 3, :] = means[:, col]
            scr[base + 3 : base + 6, :] = scales[:, col]
            scr[base + 6 : base + 10, :] = quats[:, col]
            for v in range(VIEWS_DEV):
                scr[base + 10 + 2 * v : base + 12 + 2 * v, :] = grad[v, :, col]
            scr[base + 18 : base + 22, :] = seen[:, col].astype(jnp.float32)

        def comp(r):
            return scr[pl.ds(r, 8, stride=width), :]

        m = [comp(i) for i in range(3)]
        sc = [comp(3 + i) for i in range(3)]
        q = [comp(6 + i) for i in range(4)]
        norm = q[0] * q[0] + q[1] * q[1] + q[2] * q[2] + q[3] * q[3]
        inv = 1.0 / jnp.sqrt(norm + 0.25)
        w, x, y, z = (c * inv for c in q)
        rq = [
            [1 - 2 * (y * y + z * z), 2 * (x * y - w * z), 2 * (x * z + w * y)],
            [2 * (x * y + w * z), 1 - 2 * (x * x + z * z), 2 * (y * z - w * x)],
            [2 * (x * z - w * y), 2 * (y * z + w * x), 1 - 2 * (x * x + y * y)],
        ]
        factor = [[rq[i][j] * sc[j] for j in range(3)] for i in range(3)]
        gmax = jnp.zeros((8, LANES), jnp.float32)
        lmax = jnp.zeros((8, LANES), jnp.float32)
        for v in range(VIEWS_DEV):
            r = [[rot[i, v, j] for j in range(3)] for i in range(3)]
            f = focal[0, v]
            p = [r[i][0] * m[0] + r[i][1] * m[1] + r[i][2] * m[2] + trans[v, i] for i in range(3)]
            over = 1.0 / jnp.maximum(p[2], 1.0)
            j00 = f * over
            j02 = -(j00 * p[0]) * over
            j12 = -(j00 * p[1]) * over
            first = [j00 * r[0][j] + j02 * r[2][j] for j in range(3)]
            second = [j00 * r[1][j] + j12 * r[2][j] for j in range(3)]
            pr = [sum(first[j] * factor[j][k] for j in range(3)) for k in range(3)]
            qr = [sum(second[j] * factor[j][k] for j in range(3)) for k in range(3)]
            a = pr[0] * pr[0] + pr[1] * pr[1] + pr[2] * pr[2] + 0.3
            c = qr[0] * qr[0] + qr[1] * qr[1] + qr[2] * qr[2] + 0.3
            b = pr[0] * qr[0] + pr[1] * qr[1] + pr[2] * qr[2]
            half = 0.5 * (a - c)
            lam = 0.5 * (a + c) + jnp.sqrt(half * half + b * b + 0.01)
            vis = comp(18 + v)
            g0 = comp(10 + 2 * v)
            g1 = comp(11 + 2 * v)
            gmax = jnp.maximum(gmax, (g0 * g0 + g1 * g1) * vis)
            lmax = jnp.maximum(lmax, lam * vis)
        rows = pl.ds(pl.multiple_of(g * 8, 8), 8)
        out_ref[0, rows, :] = gmax
        out_ref[1, rows, :] = lmax
        return carry

    lax.fori_loop(0, G_DEV // 1024, group, 0)


def blocks_before(counts, upto):
    total = jnp.int32(0)
    for t in range(SHARDS):
        total = total + jnp.where(t < upto, (counts[t, 0] + LANES - 1) // LANES, 0)
    return total


def each_block(where, counts, start, index, rows, store):
    offset = blocks_before(counts, where[1])

    def place_of(block):
        return ((offset + block) & (SHARDS - 1)) * PER + (block >> 5)

    def eight(i, carry):
        for j in range(8):
            b = i * 8 + j
            block = start[0, b] >> 7
            code = jnp.broadcast_to(index[pl.ds(b, 1), :], (8, LANES))
            tile = rows[:, pl.ds(pl.multiple_of(b * LANES, LANES), LANES)]
            packed = jnp.take_along_axis(
                tile, code & (LANES - 1), axis=1, mode="promise_in_bounds"
            )
            store(place_of(block), packed, (code & 256) != 0)
            after = jnp.minimum(block + 1, BLOCKS - 1)
            store(place_of(after), packed, (code & 512) != 0)
        return carry

    lax.fori_loop(0, BLOCKS // 8, eight, 0)


def fill_kernel(where, counts, start, index, means, scales, quats, low, high, out_ref, rows):
    view = where[0]

    @pl.when(view == 0)
    def _():
        rows[0:3, :] = means[...]
        rows[3:6, :] = scales[...]
        rows[6:8, :] = quats[0:2, :]

    @pl.when(view == 1)
    def _():
        rows[0:2, :] = quats[2:4, :]

    @pl.when(view > 1)
    def _():
        rows[0:2, :] = low[6:8, :]

    @pl.when((view > 0) & (view < 7))
    def _():
        rows[2:8, :] = high[0:6, :]

    @pl.when(view == 7)
    def _():
        rows[2:3, :] = high[0:1, :]
        rows[3:8, :] = jnp.zeros((5, G_DEV), jnp.float32)

    zero = jnp.zeros((8, LANES), jnp.float32)
    for i in range(BLOCKS):
        out_ref[i] = zero

    def store(at, packed, mask):
        pltpu.store(out_ref.at[at], packed, mask=mask)

    each_block(where, counts, start, index, rows, store)


def peak_kernel(where, counts, start, index, sq0, sq1, sq2, sq3, filled, out_ref, peak_ref, rows):
    for i in range(BLOCKS):
        out_ref[i] = filled[i]

    for g in range(BLOCKS // 8):
        at = slice(8 * g, 8 * g + 8)

        def top(k):
            return jnp.maximum(
                jnp.maximum(sq0[k, at, :], sq1[k, at, :]), jnp.maximum(sq2[k, at, :], sq3[k, at, :])
            )

        norm = jnp.sqrt(top(0))
        radius = 3.0 * jnp.sqrt(top(1))
        for j in range(8):
            col = slice((8 * g + j) * LANES, (8 * g + j + 1) * LANES)
            peak_ref[0:1, col] = norm[j : j + 1, :]
            peak_ref[1:2, col] = radius[j : j + 1, :]

    @pl.when(where[0] == 7)
    def _():
        rows[3:5, :] = peak_ref[...]
        sub = lax.broadcasted_iota(jnp.int32, (8, LANES), 0)
        ours = (sub == 3) | (sub == 4)

        def store(at, packed, mask):
            pltpu.store(out_ref.at[at], packed, mask=mask & ours)

        each_block(where, counts, start, index, rows, store)


def place_kernel(where, counts, arrived, out_ref, slots):
    cap = out_ref.shape[1]
    mine = where[1]
    zero = jnp.zeros((8, LANES), jnp.float32)
    for i in range(cap):
        slots[i] = zero
    before = jnp.int32(0)
    for s in range(SHARDS):
        local = (mine - before) & (SHARDS - 1)
        first = (before + local) >> 5
        for w in range(PER):
            slots[jnp.minimum(first + w, cap)] = arrived[s * PER + w]
        before = before + (counts[s, 0] + LANES - 1) // LANES
    for i in range(cap):
        tile = slots[i]
        for x in range(4):
            out_ref[x, i] = tile


def join_kernel(where, own, other, out_ref):
    cap = own.shape[1]
    core = where[0] & 1
    mine = pl.ds(pl.multiple_of(8 * core, 8), 8)
    theirs = pl.ds(pl.multiple_of(8 - 8 * core, 8), 8)
    for i in range(BLOCKS):
        col = slice(i * LANES, (i + 1) * LANES)
        if i < cap:
            out_ref[mine, col] = own[0, i]
            out_ref[theirs, col] = other[0, i]
        else:
            out_ref[:, col] = jnp.zeros((16, LANES), jnp.float32)


def smem():
    return pl.BlockSpec(memory_space=SMEM)


def vmem():
    return pl.BlockSpec(memory_space=VMEM)


def body(means, scales, quats, attrs, grad_screen, visible, clone_mask, rotation, shift, focal):
    f32, i32 = jnp.float32, jnp.int32
    view = lax.axis_index("view")
    where = jnp.stack([view, lax.axis_index("gauss")]).astype(i32)

    def whole(*shape):
        return pl.BlockSpec(shape, lambda i, w: (0,) * len(shape))

    mask = clone_mask.reshape(BLOCKS, LANES)
    count = pl.pallas_call(
        count_kernel,
        in_specs=[vmem()],
        out_specs=vmem(),
        out_shape=jax.ShapeDtypeStruct((SHARDS, LANES), i32),
        name="count",
    )(mask)
    counts = lax.all_to_all(count, "gauss", 0, 0, tiled=True)

    squares = pl.pallas_call(
        view_kernel,
        in_specs=[smem()] * 3 + [vmem()] * 5,
        out_specs=vmem(),
        out_shape=jax.ShapeDtypeStruct((2, BLOCKS, LANES), f32),
        scratch_shapes=[pltpu.VMEM((192, LANES), f32)],
        name="views",
    )(
        rotation.transpose(1, 0, 2),
        shift,
        focal.reshape(1, VIEWS_DEV),
        means,
        scales,
        quats,
        grad_screen,
        visible,
    )
    other = lax.ppermute(squares, "view", [(v, v ^ 1) for v in range(8)])
    squares = [jnp.maximum(squares, other)]
    for k in (1, 2, 3):
        pairs = [(v, (v + 2 * k) % 8) for v in range(8)]
        squares.append(lax.ppermute(squares[0], "view", pairs))

    start, index = pl.pallas_call(
        index_kernel,
        in_specs=[vmem()],
        out_specs=[vmem()] * 2,
        out_shape=[
            jax.ShapeDtypeStruct((8, LANES), i32),
            jax.ShapeDtypeStruct((BLOCKS, LANES), i32),
        ],
        name="index",
    )(mask)
    filled = pl.pallas_call(
        fill_kernel,
        grid_spec=pltpu.PrefetchScalarGridSpec(
            num_scalar_prefetch=1,
            grid=(1,),
            in_specs=[
                smem(),
                smem(),
                whole(BLOCKS, LANES),
                whole(3, G_DEV),
                whole(3, G_DEV),
                whole(4, G_DEV),
                pl.BlockSpec((8, G_DEV), lambda i, w: (jnp.maximum(w[0] - 2, 0), 0)),
                pl.BlockSpec((8, G_DEV), lambda i, w: (jnp.maximum(w[0] - 1, 0), 0)),
            ],
            out_specs=whole(BLOCKS, 8, LANES),
            scratch_shapes=[pltpu.VMEM((8, G_DEV), f32)],
        ),
        out_shape=jax.ShapeDtypeStruct((BLOCKS, 8, LANES), f32),
        name="fill",
    )(where, counts, start, index, means, scales, quats, attrs, attrs)
    outgoing, peak = pl.pallas_call(
        peak_kernel,
        in_specs=[smem()] * 3 + [vmem()] * 6,
        out_specs=[vmem()] * 2,
        out_shape=[
            jax.ShapeDtypeStruct((BLOCKS, 8, LANES), f32),
            jax.ShapeDtypeStruct((2, G_DEV), f32),
        ],
        scratch_shapes=[pltpu.VMEM((8, G_DEV), f32)],
        name="peaks",
    )(where, counts, start, index, *squares, filled)

    arrived = lax.all_to_all(
        outgoing.reshape(SHARDS, PER, 8, LANES), "gauss", 0, 0, tiled=True
    ).reshape(BLOCKS, 8, LANES)

    cap = BLOCKS
    piece = pl.pallas_call(
        place_kernel,
        in_specs=[smem(), smem(), vmem()],
        out_specs=vmem(),
        out_shape=jax.ShapeDtypeStruct((4, cap, 8, LANES), f32),
        scratch_shapes=[pltpu.VMEM((cap + 1, 8, LANES), f32)],
        name="place",
    )(where, counts, arrived)
    cores = [[0, 2, 4, 6], [1, 3, 5, 7]]
    own = lax.all_to_all(piece, "view", 0, 0, axis_index_groups=cores, tiled=True)
    other = lax.ppermute(own, "view", [(v, v ^ 1) for v in range(8)])
    clones = pl.pallas_call(
        join_kernel,
        grid_spec=pltpu.PrefetchScalarGridSpec(
            num_scalar_prefetch=1,
            grid=(4,),
            in_specs=[
                pl.BlockSpec((1, cap, 8, LANES), lambda i, w: (i, 0, 0, 0)),
                pl.BlockSpec((1, cap, 8, LANES), lambda i, w: (i, 0, 0, 0)),
            ],
            out_specs=pl.BlockSpec((16, G_DEV), lambda i, w: (i, 0)),
        ),
        out_shape=jax.ShapeDtypeStruct((ROWS, G_DEV), f32),
        name="join",
    )(where, own, other)
    return (peak, clones, jnp.sum(counts[:, 0]))


def solution(mesh):
    return jax.shard_map(
        body,
        mesh=mesh,
        in_specs=(
            P(None, "gauss"),
            P(None, "gauss"),
            P(None, "gauss"),
            P(None, "gauss"),
            P("view", None, "gauss"),
            P("view", "gauss"),
            P("gauss"),
            P("view", None, None),
            P("view", None),
            P("view"),
        ),
        out_specs=(P(None, "gauss"), P(None, "gauss"), P()),
        check_vma=False,
    )
```

```python
import jax
import jax.numpy as jnp
from jax import lax
from jax.experimental import pallas as pl
from jax.experimental.pallas import tpu as pltpu
from jax.sharding import PartitionSpec as P

G_DEV = 16384
LANES = 128
BLOCKS = G_DEV // LANES
SHARDS = 32
PER = BLOCKS // SHARDS
VIEWS_DEV = 4
STEP = 16
ROWS = 61
SMEM = pltpu.MemorySpace.SMEM
VMEM = pltpu.MemorySpace.VMEM


def dot(a, b, dims=((1,), (0,))):
    return lax.dot_general(a, b, (dims, ((), ())), preferred_element_type=jnp.float32)


def where_1(cond):
    return jnp.where(cond, 1.0, 0.0).astype(jnp.bfloat16)


def count_kernel(mask_ref, count_ref):
    total = jnp.sum(jnp.sum(mask_ref[...], axis=0, keepdims=True), axis=1, keepdims=True)
    count_ref[...] = jnp.broadcast_to(total, (SHARDS, LANES))


def index_kernel(mask_ref, start_ref, index_ref):
    marked = mask_ref[...]
    ones = marked.astype(jnp.float32).astype(jnp.bfloat16)
    row = lax.broadcasted_iota(jnp.int32, (LANES, LANES), 0)
    lane = lax.broadcasted_iota(jnp.int32, (LANES, LANES), 1)
    full = jnp.ones((LANES, LANES), jnp.bfloat16)

    inclusive = dot(ones, where_1(row <= lane)).astype(jnp.int32)
    in_row = dot(ones, full)
    start = dot(where_1(row > lane), in_row.astype(jnp.bfloat16)).astype(jnp.int32)
    in_row_t = dot(jnp.ones((8, LANES), jnp.bfloat16), ones, ((1,), (1,)))
    start_ref[...] = dot(in_row_t.astype(jnp.bfloat16), where_1(row < lane)).astype(jnp.int32)

    moves = lane - inclusive + 1
    code = jnp.where(marked == 1, moves * 256 + lane, 0)
    for bit in range(7):
        moved = pltpu.roll(code, LANES - (1 << bit), 1)
        take = ((moved >> (8 + bit)) & 1) == 1
        leave = ((code >> (8 + bit)) & 1) == 1
        code = jnp.where(take, moved, jnp.where(leave, 0, code))
    first = start & (LANES - 1)
    nth = (lane - first) & (LANES - 1)
    source = jnp.take_along_axis(
        code & (LANES - 1), nth, axis=1, mode="promise_in_bounds"
    )
    valid = nth < in_row.astype(jnp.int32)
    here = jnp.where(valid, jnp.where(lane >= first, 256, 512), 0)
    index_ref[...] = source + here


def view_kernel(rot, trans, focal, means, scales, quats, grad, seen, out_ref, scr):
    width = 23

    def group(g, carry):
        for j in range(8):
            col = pl.ds(pl.multiple_of(g * 1024 + j * LANES, LANES), LANES)
            base = j * width
            scr[base : base + 3, :] = means[:, col]
            scr[base + 3 : base + 6, :] = scales[:, col]
            scr[base + 6 : base + 10, :] = quats[:, col]
            for v in range(VIEWS_DEV):
                scr[base + 10 + 2 * v : base + 12 + 2 * v, :] = grad[v, :, col]
            scr[base + 18 : base + 22, :] = seen[:, col].astype(jnp.float32)

        def comp(r):
            return scr[pl.ds(r, 8, stride=width), :]

        m = [comp(i) for i in range(3)]
        sc = [comp(3 + i) for i in range(3)]
        q = [comp(6 + i) for i in range(4)]
        norm = q[0] * q[0] + q[1] * q[1] + q[2] * q[2] + q[3] * q[3]
        inv = 1.0 / jnp.sqrt(norm + 0.25)
        w, x, y, z = (c * inv for c in q)
        rq = [
            [1 - 2 * (y * y + z * z), 2 * (x * y - w * z), 2 * (x * z + w * y)],
            [2 * (x * y + w * z), 1 - 2 * (x * x + z * z), 2 * (y * z - w * x)],
            [2 * (x * z - w * y), 2 * (y * z + w * x), 1 - 2 * (x * x + y * y)],
        ]
        factor = [[rq[i][j] * sc[j] for j in range(3)] for i in range(3)]
        gmax = jnp.zeros((8, LANES), jnp.float32)
        lmax = jnp.zeros((8, LANES), jnp.float32)
        for v in range(VIEWS_DEV):
            r = [[rot[i, v, j] for j in range(3)] for i in range(3)]
            f = focal[0, v]
            p = [r[i][0] * m[0] + r[i][1] * m[1] + r[i][2] * m[2] + trans[v, i] for i in range(3)]
            over = 1.0 / jnp.maximum(p[2], 1.0)
            j00 = f * over
            j02 = -(j00 * p[0]) * over
            j12 = -(j00 * p[1]) * over
            first = [j00 * r[0][j] + j02 * r[2][j] for j in range(3)]
            second = [j00 * r[1][j] + j12 * r[2][j] for j in range(3)]
            pr = [sum(first[j] * factor[j][k] for j in range(3)) for k in range(3)]
            qr = [sum(second[j] * factor[j][k] for j in range(3)) for k in range(3)]
            a = pr[0] * pr[0] + pr[1] * pr[1] + pr[2] * pr[2] + 0.3
            c = qr[0] * qr[0] + qr[1] * qr[1] + qr[2] * qr[2] + 0.3
            b = pr[0] * qr[0] + pr[1] * qr[1] + pr[2] * qr[2]
            half = 0.5 * (a - c)
            lam = 0.5 * (a + c) + jnp.sqrt(half * half + b * b + 0.01)
            vis = comp(18 + v)
            g0 = comp(10 + 2 * v)
            g1 = comp(11 + 2 * v)
            gmax = jnp.maximum(gmax, (g0 * g0 + g1 * g1) * vis)
            lmax = jnp.maximum(lmax, lam * vis)
        rows = pl.ds(pl.multiple_of(g * 8, 8), 8)
        out_ref[0, rows, :] = gmax
        out_ref[1, rows, :] = lmax
        return carry

    lax.fori_loop(0, G_DEV // 1024, group, 0)


def blocks_before(counts, upto):
    total = jnp.int32(0)
    for t in range(SHARDS):
        total = total + jnp.where(t < upto, (counts[t, 0] + LANES - 1) // LANES, 0)
    return total


def each_block(where, counts, start, index, rows, store):
    offset = blocks_before(counts, where[1])

    def place_of(block):
        return ((offset + block) & (SHARDS - 1)) * PER + (block >> 5)

    def eight(i, carry):
        for j in range(8):
            b = i * 8 + j
            block = start[0, b] >> 7
            code = jnp.broadcast_to(index[pl.ds(b, 1), :], (8, LANES))
            tile = rows[:, pl.ds(pl.multiple_of(b * LANES, LANES), LANES)]
            packed = jnp.take_along_axis(
                tile, code & (LANES - 1), axis=1, mode="promise_in_bounds"
            )
            store(place_of(block), packed, (code & 256) != 0)
            after = jnp.minimum(block + 1, BLOCKS - 1)
            store(place_of(after), packed, (code & 512) != 0)
        return carry

    lax.fori_loop(0, BLOCKS // 8, eight, 0)


def fill_kernel(where, counts, start, index, means, scales, quats, low, high, out_ref, rows):
    view = where[0]

    @pl.when(view == 0)
    def _():
        rows[0:3, :] = means[...]
        rows[3:6, :] = scales[...]
        rows[6:8, :] = quats[0:2, :]

    @pl.when(view == 1)
    def _():
        rows[0:2, :] = quats[2:4, :]

    @pl.when(view > 1)
    def _():
        rows[0:2, :] = low[6:8, :]

    @pl.when((view > 0) & (view < 7))
    def _():
        rows[2:8, :] = high[0:6, :]

    @pl.when(view == 7)
    def _():
        rows[2:3, :] = high[0:1, :]
        rows[3:8, :] = jnp.zeros((5, G_DEV), jnp.float32)

    zero = jnp.zeros((8, LANES), jnp.float32)
    for i in range(BLOCKS):
        out_ref[i] = zero

    def store(at, packed, mask):
        pltpu.store(out_ref.at[at], packed, mask=mask)

    each_block(where, counts, start, index, rows, store)


def peak_kernel(where, counts, start, index, sq0, sq1, sq2, sq3, filled, out_ref, peak_ref, rows):
    for i in range(BLOCKS):
        out_ref[i] = filled[i]

    for g in range(BLOCKS // 8):
        at = slice(8 * g, 8 * g + 8)

        def top(k):
            return jnp.maximum(
                jnp.maximum(sq0[k, at, :], sq1[k, at, :]), jnp.maximum(sq2[k, at, :], sq3[k, at, :])
            )

        norm = jnp.sqrt(top(0))
        radius = 3.0 * jnp.sqrt(top(1))
        for j in range(8):
            col = slice((8 * g + j) * LANES, (8 * g + j + 1) * LANES)
            peak_ref[0:1, col] = norm[j : j + 1, :]
            peak_ref[1:2, col] = radius[j : j + 1, :]

    @pl.when(where[0] == 7)
    def _():
        rows[3:5, :] = peak_ref[...]
        sub = lax.broadcasted_iota(jnp.int32, (8, LANES), 0)
        ours = (sub == 3) | (sub == 4)

        def store(at, packed, mask):
            pltpu.store(out_ref.at[at], packed, mask=mask & ours)

        each_block(where, counts, start, index, rows, store)


def place_kernel(where, counts, arrived, out_ref, slots):
    cap = out_ref.shape[1]
    mine = where[1]
    zero = jnp.zeros((8, LANES), jnp.float32)
    for i in range(cap):
        slots[i] = zero
    before = jnp.int32(0)
    for s in range(SHARDS):
        local = (mine - before) & (SHARDS - 1)
        first = (before + local) >> 5
        for w in range(PER):
            slots[jnp.minimum(first + w, cap)] = arrived[s * PER + w]
        before = before + (counts[s, 0] + LANES - 1) // LANES
    for i in range(cap):
        tile = slots[i]
        for x in range(4):
            out_ref[x, i] = tile


def join_kernel(where, own, other, out_ref):
    cap = own.shape[1]
    core = where[0] & 1
    mine = pl.ds(pl.multiple_of(8 * core, 8), 8)
    theirs = pl.ds(pl.multiple_of(8 - 8 * core, 8), 8)
    for i in range(BLOCKS):
        col = slice(i * LANES, (i + 1) * LANES)
        if i < cap:
            out_ref[mine, col] = own[0, i]
            out_ref[theirs, col] = other[0, i]
        else:
            out_ref[:, col] = jnp.zeros((16, LANES), jnp.float32)


def smem():
    return pl.BlockSpec(memory_space=SMEM)


def vmem():
    return pl.BlockSpec(memory_space=VMEM)


def body(means, scales, quats, attrs, grad_screen, visible, clone_mask, rotation, shift, focal):
    f32, i32 = jnp.float32, jnp.int32
    view = lax.axis_index("view")
    where = jnp.stack([view, lax.axis_index("gauss")]).astype(i32)

    def whole(*shape):
        return pl.BlockSpec(shape, lambda i, w: (0,) * len(shape))

    mask = clone_mask.reshape(BLOCKS, LANES)
    count = pl.pallas_call(
        count_kernel,
        in_specs=[vmem()],
        out_specs=vmem(),
        out_shape=jax.ShapeDtypeStruct((SHARDS, LANES), i32),
        name="count",
    )(mask)
    counts = lax.all_to_all(count, "gauss", 0, 0, tiled=True)

    squares = pl.pallas_call(
        view_kernel,
        in_specs=[smem()] * 3 + [vmem()] * 5,
        out_specs=vmem(),
        out_shape=jax.ShapeDtypeStruct((2, BLOCKS, LANES), f32),
        scratch_shapes=[pltpu.VMEM((192, LANES), f32)],
        name="views",
    )(
        rotation.transpose(1, 0, 2),
        shift,
        focal.reshape(1, VIEWS_DEV),
        means,
        scales,
        quats,
        grad_screen,
        visible,
    )
    other = lax.ppermute(squares, "view", [(v, v ^ 1) for v in range(8)])
    squares = [jnp.maximum(squares, other)]
    for k in (1, 2, 3):
        pairs = [(v, (v + 2 * k) % 8) for v in range(8)]
        squares.append(lax.ppermute(squares[0], "view", pairs))

    start, index = pl.pallas_call(
        index_kernel,
        in_specs=[vmem()],
        out_specs=[vmem()] * 2,
        out_shape=[
            jax.ShapeDtypeStruct((8, LANES), i32),
            jax.ShapeDtypeStruct((BLOCKS, LANES), i32),
        ],
        name="index",
    )(mask)
    filled = pl.pallas_call(
        fill_kernel,
        grid_spec=pltpu.PrefetchScalarGridSpec(
            num_scalar_prefetch=1,
            grid=(1,),
            in_specs=[
                smem(),
                smem(),
                whole(BLOCKS, LANES),
                whole(3, G_DEV),
                whole(3, G_DEV),
                whole(4, G_DEV),
                pl.BlockSpec((8, G_DEV), lambda i, w: (jnp.maximum(w[0] - 2, 0), 0)),
                pl.BlockSpec((8, G_DEV), lambda i, w: (jnp.maximum(w[0] - 1, 0), 0)),
            ],
            out_specs=whole(BLOCKS, 8, LANES),
            scratch_shapes=[pltpu.VMEM((8, G_DEV), f32)],
        ),
        out_shape=jax.ShapeDtypeStruct((BLOCKS, 8, LANES), f32),
        name="fill",
    )(where, counts, start, index, means, scales, quats, attrs, attrs)
    outgoing, peak = pl.pallas_call(
        peak_kernel,
        in_specs=[smem()] * 3 + [vmem()] * 6,
        out_specs=[vmem()] * 2,
        out_shape=[
            jax.ShapeDtypeStruct((BLOCKS, 8, LANES), f32),
            jax.ShapeDtypeStruct((2, G_DEV), f32),
        ],
        scratch_shapes=[pltpu.VMEM((8, G_DEV), f32)],
        name="peaks",
    )(where, counts, start, index, *squares, filled)

    arrived = lax.all_to_all(
        outgoing.reshape(SHARDS, PER, 8, LANES), "gauss", 0, 0, tiled=True
    ).reshape(BLOCKS, 8, LANES)

    used = jnp.sum((counts[:, 0] + LANES - 1) >> 7)
    rounds = (used + SHARDS * STEP - 1) >> 9

    def gather(cap):
        def go(where, counts, arrived):
            piece = pl.pallas_call(
                place_kernel,
                in_specs=[smem(), smem(), vmem()],
                out_specs=vmem(),
                out_shape=jax.ShapeDtypeStruct((4, cap, 8, LANES), f32),
                scratch_shapes=[pltpu.VMEM((cap + 1, 8, LANES), f32)],
                name="place",
            )(where, counts, arrived)
            cores = [[0, 2, 4, 6], [1, 3, 5, 7]]
            own = lax.all_to_all(piece, "view", 0, 0, axis_index_groups=cores, tiled=True)
            other = lax.ppermute(own, "view", [(v, v ^ 1) for v in range(8)])
            return pl.pallas_call(
                join_kernel,
                grid_spec=pltpu.PrefetchScalarGridSpec(
                    num_scalar_prefetch=1,
                    grid=(4,),
                    in_specs=[
                        pl.BlockSpec((1, cap, 8, LANES), lambda i, w: (i, 0, 0, 0)),
                        pl.BlockSpec((1, cap, 8, LANES), lambda i, w: (i, 0, 0, 0)),
                    ],
                    out_specs=pl.BlockSpec((16, G_DEV), lambda i, w: (i, 0)),
                ),
                out_shape=jax.ShapeDtypeStruct((ROWS, G_DEV), f32),
                name="join",
            )(where, own, other)

        return go

    clones = lax.switch(
        jnp.clip(rounds - 1, 0, BLOCKS // STEP - 1),
        [gather(cap) for cap in range(STEP, BLOCKS + 1, STEP)],
        where,
        counts,
        arrived,
    )
    return (peak, clones, jnp.sum(counts[:, 0]))


def solution(mesh):
    return jax.shard_map(
        body,
        mesh=mesh,
        in_specs=(
            P(None, "gauss"),
            P(None, "gauss"),
            P(None, "gauss"),
            P(None, "gauss"),
            P("view", None, "gauss"),
            P("view", "gauss"),
            P("gauss"),
            P("view", None, None),
            P("view", None),
            P("view"),
        ),
        out_specs=(P(None, "gauss"), P(None, "gauss"), P()),
        check_vma=False,
    )
```

```python
import jax
import jax.numpy as jnp
from jax import lax
from jax.experimental import pallas as pl
from jax.experimental.pallas import tpu as pltpu
from jax.sharding import PartitionSpec as P

G_DEV = 16384
LANES = 128
BLOCKS = G_DEV // LANES
SHARDS = 32
PER = BLOCKS // SHARDS
VIEWS_DEV = 4
STEP = 16
ROWS = 61
LIMIT = pltpu.CompilerParams(vmem_limit_bytes=16 * 2**20)
SMEM = pltpu.MemorySpace.SMEM
VMEM = pltpu.MemorySpace.VMEM


def dot(a, b, dims=((1,), (0,))):
    return lax.dot_general(a, b, (dims, ((), ())), preferred_element_type=jnp.float32)


def where_1(cond):
    return jnp.where(cond, 1.0, 0.0).astype(jnp.bfloat16)


def count_kernel(mask_ref, count_ref):
    total = jnp.sum(jnp.sum(mask_ref[...], axis=0, keepdims=True), axis=1, keepdims=True)
    count_ref[...] = jnp.broadcast_to(total, (SHARDS, LANES))


def index_kernel(mask_ref, start_ref, index_ref):
    marked = mask_ref[...]
    ones = marked.astype(jnp.float32).astype(jnp.bfloat16)
    row = lax.broadcasted_iota(jnp.int32, (LANES, LANES), 0)
    lane = lax.broadcasted_iota(jnp.int32, (LANES, LANES), 1)
    full = jnp.ones((LANES, LANES), jnp.bfloat16)

    inclusive = dot(ones, where_1(row <= lane)).astype(jnp.int32)
    in_row = dot(ones, full)
    start = dot(where_1(row > lane), in_row.astype(jnp.bfloat16)).astype(jnp.int32)
    in_row_t = dot(jnp.ones((8, LANES), jnp.bfloat16), ones, ((1,), (1,)))
    start_ref[...] = dot(in_row_t.astype(jnp.bfloat16), where_1(row < lane)).astype(jnp.int32)

    moves = lane - inclusive + 1
    code = jnp.where(marked == 1, moves * 256 + lane, 0)
    for bit in range(7):
        moved = pltpu.roll(code, LANES - (1 << bit), 1)
        take = ((moved >> (8 + bit)) & 1) == 1
        leave = ((code >> (8 + bit)) & 1) == 1
        code = jnp.where(take, moved, jnp.where(leave, 0, code))
    first = start & (LANES - 1)
    nth = (lane - first) & (LANES - 1)
    source = jnp.take_along_axis(
        code & (LANES - 1), nth, axis=1, mode="promise_in_bounds"
    )
    valid = nth < in_row.astype(jnp.int32)
    here = jnp.where(valid, jnp.where(lane >= first, 256, 512), 0)
    index_ref[...] = source + here


def view_kernel(rot, trans, focal, means, scales, quats, grad, seen, out_ref, scr):
    width = 23

    def group(g, carry):
        for j in range(8):
            col = pl.ds(pl.multiple_of(g * 1024 + j * LANES, LANES), LANES)
            base = j * width
            scr[base : base + 3, :] = means[:, col]
            scr[base + 3 : base + 6, :] = scales[:, col]
            scr[base + 6 : base + 10, :] = quats[:, col]
            for v in range(VIEWS_DEV):
                scr[base + 10 + 2 * v : base + 12 + 2 * v, :] = grad[v, :, col]
            scr[base + 18 : base + 22, :] = seen[:, col].astype(jnp.float32)

        def comp(r):
            return scr[pl.ds(r, 8, stride=width), :]

        m = [comp(i) for i in range(3)]
        sc = [comp(3 + i) for i in range(3)]
        q = [comp(6 + i) for i in range(4)]
        norm = q[0] * q[0] + q[1] * q[1] + q[2] * q[2] + q[3] * q[3]
        inv = 1.0 / jnp.sqrt(norm + 0.25)
        w, x, y, z = (c * inv for c in q)
        rq = [
            [1 - 2 * (y * y + z * z), 2 * (x * y - w * z), 2 * (x * z + w * y)],
            [2 * (x * y + w * z), 1 - 2 * (x * x + z * z), 2 * (y * z - w * x)],
            [2 * (x * z - w * y), 2 * (y * z + w * x), 1 - 2 * (x * x + y * y)],
        ]
        factor = [[rq[i][j] * sc[j] for j in range(3)] for i in range(3)]
        gmax = jnp.zeros((8, LANES), jnp.float32)
        lmax = jnp.zeros((8, LANES), jnp.float32)
        for v in range(VIEWS_DEV):
            r = [[rot[i, v, j] for j in range(3)] for i in range(3)]
            f = focal[0, v]
            p = [r[i][0] * m[0] + r[i][1] * m[1] + r[i][2] * m[2] + trans[v, i] for i in range(3)]
            over = 1.0 / jnp.maximum(p[2], 1.0)
            j00 = f * over
            j02 = -(j00 * p[0]) * over
            j12 = -(j00 * p[1]) * over
            first = [j00 * r[0][j] + j02 * r[2][j] for j in range(3)]
            second = [j00 * r[1][j] + j12 * r[2][j] for j in range(3)]
            pr = [sum(first[j] * factor[j][k] for j in range(3)) for k in range(3)]
            qr = [sum(second[j] * factor[j][k] for j in range(3)) for k in range(3)]
            a = pr[0] * pr[0] + pr[1] * pr[1] + pr[2] * pr[2] + 0.3
            c = qr[0] * qr[0] + qr[1] * qr[1] + qr[2] * qr[2] + 0.3
            b = pr[0] * qr[0] + pr[1] * qr[1] + pr[2] * qr[2]
            half = 0.5 * (a - c)
            lam = 0.5 * (a + c) + jnp.sqrt(half * half + b * b + 0.01)
            vis = comp(18 + v)
            g0 = comp(10 + 2 * v)
            g1 = comp(11 + 2 * v)
            gmax = jnp.maximum(gmax, (g0 * g0 + g1 * g1) * vis)
            lmax = jnp.maximum(lmax, lam * vis)
        rows = pl.ds(pl.multiple_of(g * 8, 8), 8)
        out_ref[0, rows, :] = gmax
        out_ref[1, rows, :] = lmax
        return carry

    lax.fori_loop(0, G_DEV // 1024, group, 0)


def blocks_before(counts, upto):
    total = jnp.int32(0)
    for t in range(SHARDS):
        total = total + jnp.where(t < upto, (counts[t, 0] + LANES - 1) // LANES, 0)
    return total


def each_block(where, counts, start, index, rows, store):
    offset = blocks_before(counts, where[1])

    def place_of(block):
        return ((offset + block) & (SHARDS - 1)) * PER + (block >> 5)

    def eight(i, carry):
        for j in range(8):
            b = i * 8 + j
            block = start[0, b] >> 7
            code = jnp.broadcast_to(index[pl.ds(b, 1), :], (8, LANES))
            tile = rows[:, pl.ds(pl.multiple_of(b * LANES, LANES), LANES)]
            packed = jnp.take_along_axis(
                tile, code & (LANES - 1), axis=1, mode="promise_in_bounds"
            )
            store(place_of(block), packed, (code & 256) != 0)
            after = jnp.minimum(block + 1, BLOCKS - 1)
            store(place_of(after), packed, (code & 512) != 0)
        return carry

    lax.fori_loop(0, BLOCKS // 8, eight, 0)


def fill_kernel(where, counts, start, index, means, scales, quats, low, high, out_ref, rows):
    view = where[0]

    @pl.when(view == 0)
    def _():
        rows[0:3, :] = means[...]
        rows[3:6, :] = scales[...]
        rows[6:8, :] = quats[0:2, :]

    @pl.when(view == 1)
    def _():
        rows[0:2, :] = quats[2:4, :]

    @pl.when(view > 1)
    def _():
        rows[0:2, :] = low[6:8, :]

    @pl.when((view > 0) & (view < 7))
    def _():
        rows[2:8, :] = high[0:6, :]

    @pl.when(view == 7)
    def _():
        rows[2:3, :] = high[0:1, :]
        rows[3:8, :] = jnp.zeros((5, G_DEV), jnp.float32)

    zero = jnp.zeros((8, LANES), jnp.float32)
    for i in range(BLOCKS):
        out_ref[i] = zero

    def store(at, packed, mask):
        pltpu.store(out_ref.at[at], packed, mask=mask)

    each_block(where, counts, start, index, rows, store)


def peak_kernel(where, counts, start, index, sq0, sq1, sq2, sq3, filled, out_ref, peak_ref, rows):
    for i in range(BLOCKS):
        out_ref[i] = filled[i]

    for g in range(BLOCKS // 8):
        at = slice(8 * g, 8 * g + 8)

        def top(k):
            return jnp.maximum(
                jnp.maximum(sq0[k, at, :], sq1[k, at, :]), jnp.maximum(sq2[k, at, :], sq3[k, at, :])
            )

        norm = jnp.sqrt(top(0))
        radius = 3.0 * jnp.sqrt(top(1))
        for j in range(8):
            col = slice((8 * g + j) * LANES, (8 * g + j + 1) * LANES)
            peak_ref[0:1, col] = norm[j : j + 1, :]
            peak_ref[1:2, col] = radius[j : j + 1, :]

    @pl.when(where[0] == 7)
    def _():
        rows[3:5, :] = peak_ref[...]
        sub = lax.broadcasted_iota(jnp.int32, (8, LANES), 0)
        ours = (sub == 3) | (sub == 4)

        def store(at, packed, mask):
            pltpu.store(out_ref.at[at], packed, mask=mask & ours)

        each_block(where, counts, start, index, rows, store)


def place_kernel(where, counts, arrived, out_ref, slots):
    cap = out_ref.shape[1]
    mine = where[1]
    zero = jnp.zeros((8, LANES), jnp.float32)
    for i in range(cap):
        slots[i] = zero
    before = jnp.int32(0)
    for s in range(SHARDS):
        local = (mine - before) & (SHARDS - 1)
        first = (before + local) >> 5
        for w in range(PER):
            slots[jnp.minimum(first + w, cap)] = arrived[s * PER + w]
        before = before + (counts[s, 0] + LANES - 1) // LANES
    for i in range(cap):
        tile = slots[i]
        for x in range(4):
            out_ref[x, i] = tile


def join_kernel(where, own, other, out_ref):
    cap = own.shape[1]
    core = where[0] & 1
    mine = pl.ds(pl.multiple_of(8 * core, 8), 8)
    theirs = pl.ds(pl.multiple_of(8 - 8 * core, 8), 8)
    for i in range(BLOCKS):
        col = slice(i * LANES, (i + 1) * LANES)
        if i < cap:
            out_ref[mine, col] = own[0, i]
            out_ref[theirs, col] = other[0, i]
        else:
            out_ref[:, col] = jnp.zeros((16, LANES), jnp.float32)


def smem():
    return pl.BlockSpec(memory_space=SMEM)


def vmem():
    return pl.BlockSpec(memory_space=VMEM)


def body(means, scales, quats, attrs, grad_screen, visible, clone_mask, rotation, shift, focal):
    f32, i32 = jnp.float32, jnp.int32
    view = lax.axis_index("view")
    where = jnp.stack([view, lax.axis_index("gauss")]).astype(i32)

    def whole(*shape):
        return pl.BlockSpec(shape, lambda i, w: (0,) * len(shape))

    mask = clone_mask.reshape(BLOCKS, LANES)
    rotation, focal = rotation.transpose(1, 0, 2), focal.reshape(1, VIEWS_DEV)
    mask, means, scales, quats, attrs, grad_screen, visible, rotation, shift, focal = (
        pltpu.with_memory_space_constraint(x, pltpu.MemorySpace.HBM)
        for x in (
            mask, means, scales, quats, attrs, grad_screen, visible, rotation, shift, focal
        )
    )
    count = pl.pallas_call(
        count_kernel,
        in_specs=[vmem()],
        out_specs=vmem(),
        out_shape=VMEM((SHARDS, LANES), i32),
        compiler_params=LIMIT,
        name="count",
    )(mask)
    counts = lax.all_to_all(count, "gauss", 0, 0, tiled=True)

    squares = pl.pallas_call(
        view_kernel,
        in_specs=[smem()] * 3 + [vmem()] * 5,
        out_specs=vmem(),
        out_shape=VMEM((2, BLOCKS, LANES), f32),
        scratch_shapes=[pltpu.VMEM((192, LANES), f32)],
        compiler_params=LIMIT,
        name="views",
    )(
        rotation,
        shift,
        focal,
        means,
        scales,
        quats,
        grad_screen,
        visible,
    )
    other = lax.ppermute(squares, "view", [(v, v ^ 1) for v in range(8)])
    squares = [jnp.maximum(squares, other)]
    for k in (1, 2, 3):
        pairs = [(v, (v + 2 * k) % 8) for v in range(8)]
        squares.append(lax.ppermute(squares[0], "view", pairs))

    start, index = pl.pallas_call(
        index_kernel,
        in_specs=[vmem()],
        out_specs=[vmem()] * 2,
        out_shape=[
            VMEM((8, LANES), i32),
            VMEM((BLOCKS, LANES), i32),
        ],
        compiler_params=LIMIT,
        name="index",
    )(mask)
    filled = pl.pallas_call(
        fill_kernel,
        grid_spec=pltpu.PrefetchScalarGridSpec(
            num_scalar_prefetch=1,
            grid=(1,),
            in_specs=[
                smem(),
                smem(),
                whole(BLOCKS, LANES),
                whole(3, G_DEV),
                whole(3, G_DEV),
                whole(4, G_DEV),
                pl.BlockSpec((8, G_DEV), lambda i, w: (jnp.maximum(w[0] - 2, 0), 0)),
                pl.BlockSpec((8, G_DEV), lambda i, w: (jnp.maximum(w[0] - 1, 0), 0)),
            ],
            out_specs=whole(BLOCKS, 8, LANES),
            scratch_shapes=[pltpu.VMEM((8, G_DEV), f32)],
        ),
        out_shape=VMEM((BLOCKS, 8, LANES), f32),
        compiler_params=LIMIT,
        name="fill",
    )(where, counts, start, index, means, scales, quats, attrs, attrs)
    outgoing, peak = pl.pallas_call(
        peak_kernel,
        in_specs=[smem()] * 3 + [vmem()] * 6,
        out_specs=[vmem()] * 2,
        out_shape=[
            VMEM((BLOCKS, 8, LANES), f32),
            jax.ShapeDtypeStruct((2, G_DEV), f32),
        ],
        scratch_shapes=[pltpu.VMEM((8, G_DEV), f32)],
        compiler_params=LIMIT,
        name="peaks",
    )(where, counts, start, index, *squares, filled)

    used = jnp.sum((counts[:, 0] + LANES - 1) >> 7)
    rounds = (used + SHARDS * STEP - 1) >> 9
    branch = jnp.clip(rounds - 1, 0, BLOCKS // STEP - 1)

    def gather(cap):
        def go(where, counts, outgoing):
            arrived = lax.all_to_all(
                outgoing.reshape(SHARDS, PER, 8, LANES), "gauss", 0, 0, tiled=True
            ).reshape(BLOCKS, 8, LANES)
            piece = pl.pallas_call(
                place_kernel,
                in_specs=[smem(), smem(), vmem()],
                out_specs=vmem(),
                out_shape=VMEM((4, cap, 8, LANES), f32),
                scratch_shapes=[pltpu.VMEM((cap + 1, 8, LANES), f32)],
                compiler_params=LIMIT,
                name="place",
            )(where, counts, arrived)
            cores = [[0, 2, 4, 6], [1, 3, 5, 7]]
            own = lax.all_to_all(piece, "view", 0, 0, axis_index_groups=cores, tiled=True)
            other = lax.ppermute(own, "view", [(v, v ^ 1) for v in range(8)])
            return pl.pallas_call(
                join_kernel,
                grid_spec=pltpu.PrefetchScalarGridSpec(
                    num_scalar_prefetch=1,
                    grid=(4,),
                    in_specs=[
                        pl.BlockSpec((1, cap, 8, LANES), lambda i, w: (i, 0, 0, 0)),
                        pl.BlockSpec((1, cap, 8, LANES), lambda i, w: (i, 0, 0, 0)),
                    ],
                    out_specs=pl.BlockSpec((16, G_DEV), lambda i, w: (i, 0)),
                ),
                out_shape=jax.ShapeDtypeStruct((ROWS, G_DEV), f32),
                compiler_params=LIMIT,
                name="join",
            )(where, own, other)

        return go

    clones = lax.switch(
        branch,
        [gather(cap) for cap in range(STEP, BLOCKS + 1, STEP)],
        where,
        counts,
        outgoing,
    )
    return (peak, clones, jnp.sum(counts[:, 0]))


def solution(mesh):
    return jax.shard_map(
        body,
        mesh=mesh,
        in_specs=(
            P(None, "gauss"),
            P(None, "gauss"),
            P(None, "gauss"),
            P(None, "gauss"),
            P("view", None, "gauss"),
            P("view", "gauss"),
            P("gauss"),
            P("view", None, None),
            P("view", None),
            P("view"),
        ),
        out_specs=(P(None, "gauss"), P(None, "gauss"), P()),
        check_vma=False,
    )
```

```python
import jax
import jax.numpy as jnp
from jax import lax
from jax.experimental import pallas as pl
from jax.experimental.pallas import tpu as pltpu
from jax.sharding import PartitionSpec as P

G_DEV = 16384
LANES = 128
BLOCKS = G_DEV // LANES
SHARDS = 32
PER = BLOCKS // SHARDS
VIEWS_DEV = 4
STEP = 16
ROWS = 61
LIMIT = pltpu.CompilerParams(vmem_limit_bytes=16 * 2**20)
SMEM = pltpu.MemorySpace.SMEM
VMEM = pltpu.MemorySpace.VMEM


def dot(a, b, dims=((1,), (0,))):
    return lax.dot_general(a, b, (dims, ((), ())), preferred_element_type=jnp.float32)


def where_1(cond):
    return jnp.where(cond, 1.0, 0.0).astype(jnp.bfloat16)


def count_kernel(mask_ref, count_ref):
    total = jnp.sum(jnp.sum(mask_ref[...], axis=0, keepdims=True), axis=1, keepdims=True)
    count_ref[...] = jnp.broadcast_to(total, (SHARDS, LANES))


def index_kernel(mask_ref, start_ref, index_ref):
    marked = mask_ref[...]
    ones = marked.astype(jnp.float32).astype(jnp.bfloat16)
    row = lax.broadcasted_iota(jnp.int32, (LANES, LANES), 0)
    lane = lax.broadcasted_iota(jnp.int32, (LANES, LANES), 1)
    full = jnp.ones((LANES, LANES), jnp.bfloat16)

    inclusive = dot(ones, where_1(row <= lane)).astype(jnp.int32)
    in_row = dot(ones, full)
    start = dot(where_1(row > lane), in_row.astype(jnp.bfloat16)).astype(jnp.int32)
    in_row_t = dot(jnp.ones((8, LANES), jnp.bfloat16), ones, ((1,), (1,)))
    start_ref[...] = dot(in_row_t.astype(jnp.bfloat16), where_1(row < lane)).astype(jnp.int32)

    moves = lane - inclusive + 1
    code = jnp.where(marked == 1, moves * 256 + lane, 0)
    for bit in range(7):
        moved = pltpu.roll(code, LANES - (1 << bit), 1)
        take = ((moved >> (8 + bit)) & 1) == 1
        leave = ((code >> (8 + bit)) & 1) == 1
        code = jnp.where(take, moved, jnp.where(leave, 0, code))
    first = start & (LANES - 1)
    nth = (lane - first) & (LANES - 1)
    source = jnp.take_along_axis(
        code & (LANES - 1), nth, axis=1, mode="promise_in_bounds"
    )
    valid = nth < in_row.astype(jnp.int32)
    here = jnp.where(valid, jnp.where(lane >= first, 256, 512), 0)
    index_ref[...] = source + here


def view_kernel(rot, trans, focal, means, scales, quats, grad, seen, out_ref, scr):
    width = 23

    def group(g, carry):
        for j in range(8):
            col = pl.ds(pl.multiple_of(g * 1024 + j * LANES, LANES), LANES)
            base = j * width
            scr[base : base + 3, :] = means[:, col]
            scr[base + 3 : base + 6, :] = scales[:, col]
            scr[base + 6 : base + 10, :] = quats[:, col]
            for v in range(VIEWS_DEV):
                scr[base + 10 + 2 * v : base + 12 + 2 * v, :] = grad[v, :, col]
            scr[base + 18 : base + 22, :] = seen[:, col].astype(jnp.float32)

        def comp(r):
            return scr[pl.ds(r, 8, stride=width), :]

        m = [comp(i) for i in range(3)]
        sc = [comp(3 + i) for i in range(3)]
        q = [comp(6 + i) for i in range(4)]
        norm = q[0] * q[0] + q[1] * q[1] + q[2] * q[2] + q[3] * q[3]
        inv = 1.0 / jnp.sqrt(norm + 0.25)
        w, x, y, z = (c * inv for c in q)
        rq = [
            [1 - 2 * (y * y + z * z), 2 * (x * y - w * z), 2 * (x * z + w * y)],
            [2 * (x * y + w * z), 1 - 2 * (x * x + z * z), 2 * (y * z - w * x)],
            [2 * (x * z - w * y), 2 * (y * z + w * x), 1 - 2 * (x * x + y * y)],
        ]
        factor = [[rq[i][j] * sc[j] for j in range(3)] for i in range(3)]
        gmax = jnp.zeros((8, LANES), jnp.float32)
        lmax = jnp.zeros((8, LANES), jnp.float32)
        for v in range(VIEWS_DEV):
            r = [[rot[i, v, j] for j in range(3)] for i in range(3)]
            f = focal[0, v]
            p = [r[i][0] * m[0] + r[i][1] * m[1] + r[i][2] * m[2] + trans[v, i] for i in range(3)]
            over = 1.0 / jnp.maximum(p[2], 1.0)
            j00 = f * over
            j02 = -(j00 * p[0]) * over
            j12 = -(j00 * p[1]) * over
            first = [j00 * r[0][j] + j02 * r[2][j] for j in range(3)]
            second = [j00 * r[1][j] + j12 * r[2][j] for j in range(3)]
            pr = [sum(first[j] * factor[j][k] for j in range(3)) for k in range(3)]
            qr = [sum(second[j] * factor[j][k] for j in range(3)) for k in range(3)]
            a = pr[0] * pr[0] + pr[1] * pr[1] + pr[2] * pr[2] + 0.3
            c = qr[0] * qr[0] + qr[1] * qr[1] + qr[2] * qr[2] + 0.3
            b = pr[0] * qr[0] + pr[1] * qr[1] + pr[2] * qr[2]
            half = 0.5 * (a - c)
            lam = 0.5 * (a + c) + jnp.sqrt(half * half + b * b + 0.01)
            vis = comp(18 + v)
            g0 = comp(10 + 2 * v)
            g1 = comp(11 + 2 * v)
            gmax = jnp.maximum(gmax, (g0 * g0 + g1 * g1) * vis)
            lmax = jnp.maximum(lmax, lam * vis)
        rows = pl.ds(pl.multiple_of(g * 8, 8), 8)
        out_ref[0, rows, :] = gmax
        out_ref[1, rows, :] = lmax
        return carry

    lax.fori_loop(0, means.shape[1] // 1024, group, 0)


def blocks_before(counts, upto):
    total = jnp.int32(0)
    for t in range(SHARDS):
        total = total + jnp.where(t < upto, (counts[t, 0] + LANES - 1) // LANES, 0)
    return total


def each_block(where, counts, start, index, rows, store):
    offset = blocks_before(counts, where[1])

    def place_of(block):
        return ((offset + block) & (SHARDS - 1)) * PER + (block >> 5)

    def eight(i, carry):
        for j in range(8):
            b = i * 8 + j
            block = start[0, b] >> 7
            code = jnp.broadcast_to(index[pl.ds(b, 1), :], (8, LANES))
            tile = rows[:, pl.ds(pl.multiple_of(b * LANES, LANES), LANES)]
            packed = jnp.take_along_axis(
                tile, code & (LANES - 1), axis=1, mode="promise_in_bounds"
            )
            store(place_of(block), packed, (code & 256) != 0)
            after = jnp.minimum(block + 1, BLOCKS - 1)
            store(place_of(after), packed, (code & 512) != 0)
        return carry

    lax.fori_loop(0, BLOCKS // 8, eight, 0)


def fill_kernel(
    where, counts, start, index, means, scales, quats, low, high, out_ref, sums_ref, pick_ref, rows
):
    view = where[0]

    @pl.when(view == 0)
    def _():
        rows[0:3, :] = means[...]
        rows[3:6, :] = scales[...]
        rows[6:8, :] = quats[0:2, :]

    @pl.when(view == 1)
    def _():
        rows[0:2, :] = quats[2:4, :]

    @pl.when(view > 1)
    def _():
        rows[0:2, :] = low[6:8, :]

    @pl.when((view > 0) & (view < 7))
    def _():
        rows[2:8, :] = high[0:6, :]

    @pl.when(view == 7)
    def _():
        rows[2:3, :] = high[0:1, :]
        rows[3:8, :] = jnp.zeros((5, G_DEV), jnp.float32)

    total = jnp.int32(0)
    for t in range(SHARDS):
        total = total + counts[t, 0]
    sums_ref[0] = total
    used = blocks_before(counts, SHARDS)
    pick_ref[0] = jnp.clip(((used + SHARDS * STEP - 1) >> 9) - 1, 0, BLOCKS // STEP - 1)

    zero = jnp.zeros((8, LANES), jnp.float32)
    for i in range(BLOCKS):
        out_ref[i] = zero

    def store(at, packed, mask):
        pltpu.store(out_ref.at[at], packed, mask=mask)

    each_block(where, counts, start, index, rows, store)


def peak_kernel(where, counts, start, index, sq0, sq1, sq2, sq3, filled, out_ref, peak_ref, pairs):
    last = where[0] == 7
    for i in range(BLOCKS):
        out_ref[i] = filled[i]

    def top(k, at):
        return jnp.maximum(
            jnp.maximum(sq0[k, at, :], sq1[k, at, :]), jnp.maximum(sq2[k, at, :], sq3[k, at, :])
        )

    for g in range(BLOCKS // 8):
        at = slice(8 * g, 8 * g + 8)
        norm = jnp.sqrt(top(0, at))
        radius = 3.0 * jnp.sqrt(top(1, at))
        pairs[pl.ds(16 * g, 8, stride=2), :] = norm
        pairs[pl.ds(16 * g + 1, 8, stride=2), :] = radius
    for b in range(BLOCKS):
        peak_ref[:, b * LANES : (b + 1) * LANES] = pairs[2 * b : 2 * b + 2, :]

    @pl.when(last)
    def _():
        offset = blocks_before(counts, where[1])

        def place_of(block):
            return ((offset + block) & (SHARDS - 1)) * PER + (block >> 5)

        def eight(g, carry):
            at = pl.ds(pl.multiple_of(g * 8, 8), 8)
            lanes = index[at, :] & (LANES - 1)
            for k in range(2):
                rows = pairs[pl.ds(16 * g + k, 8, stride=2), :]
                pairs[pl.ds(2 * BLOCKS + k, 8, stride=2), :] = jnp.take_along_axis(
                    rows, lanes, axis=1, mode="promise_in_bounds"
                )
            for j in range(8):
                b = g * 8 + j
                block = start[0, b] >> 7
                after = jnp.minimum(block + 1, BLOCKS - 1)
                code = jnp.broadcast_to(index[pl.ds(b, 1), :], (2, LANES))
                two = pairs[2 * BLOCKS + 2 * j : 2 * BLOCKS + 2 * j + 2, :]
                pltpu.store(out_ref.at[place_of(block), 3:5, :], two, mask=(code & 256) != 0)
                pltpu.store(out_ref.at[place_of(after), 3:5, :], two, mask=(code & 512) != 0)
            return carry

        lax.fori_loop(0, BLOCKS // 8, eight, 0)


def place_kernel(where, counts, arrived, out_ref, slots):
    cap = out_ref.shape[1]
    mine = where[1]
    zero = jnp.zeros((8, LANES), jnp.float32)
    for i in range(cap):
        slots[i] = zero
    before = jnp.int32(0)
    for s in range(SHARDS):
        local = (mine - before) & (SHARDS - 1)
        first = (before + local) >> 5
        for w in range(PER):
            slots[jnp.minimum(first + w, cap)] = arrived[s * PER + w]
        before = before + (counts[s, 0] + LANES - 1) // LANES
    for i in range(cap):
        tile = slots[i]
        for x in range(4):
            out_ref[x, i] = tile


def join_kernel(where, own, other, out_ref, buf, sems):
    cap = own.shape[1]
    core = where[0] & 1

    def copy(r):
        rows = min(8, ROWS - 8 * r)
        return pltpu.make_async_copy(
            buf.at[r, 0:rows, :], out_ref.at[8 * r : 8 * r + rows, :], sems.at[r]
        )

    for r in range(8):
        for half in range(2):

            @pl.when(core == half)
            def _():
                piece = own if r % 2 == half else other
                for i in range(cap):
                    buf[r, :, i * LANES : (i + 1) * LANES] = piece[r // 2, i]

        for i in range(cap, BLOCKS):
            buf[r, :, i * LANES : (i + 1) * LANES] = jnp.zeros((8, LANES), jnp.float32)
        copy(r).start()
    for r in range(8):
        copy(r).wait()


def smem():
    return pl.BlockSpec(memory_space=SMEM)


def vmem():
    return pl.BlockSpec(memory_space=VMEM)


def body(means, scales, quats, attrs, grad_screen, visible, clone_mask, rotation, shift, focal):
    f32, i32 = jnp.float32, jnp.int32
    view = lax.axis_index("view")
    where = jnp.stack([view, lax.axis_index("gauss")]).astype(i32)

    def whole(*shape):
        return pl.BlockSpec(shape, lambda i, w: (0,) * len(shape))

    mask = clone_mask.reshape(BLOCKS, LANES)
    rotation, focal = rotation.transpose(1, 0, 2), focal.reshape(1, VIEWS_DEV)
    mask, means, scales, quats, attrs, grad_screen, visible, rotation, shift, focal = (
        pltpu.with_memory_space_constraint(x, pltpu.MemorySpace.HBM)
        for x in (
            mask, means, scales, quats, attrs, grad_screen, visible, rotation, shift, focal
        )
    )
    count = pl.pallas_call(
        count_kernel,
        in_specs=[vmem()],
        out_specs=vmem(),
        out_shape=VMEM((SHARDS, LANES), i32),
        compiler_params=LIMIT,
        name="count",
    )(mask)
    counts = lax.all_to_all(count, "gauss", 0, 0, tiled=True)

    chunk = G_DEV // 4
    squares = pl.pallas_call(
        view_kernel,
        grid=(4,),
        in_specs=[smem()] * 3
        + [
            pl.BlockSpec((3, chunk), lambda i: (0, i)),
            pl.BlockSpec((3, chunk), lambda i: (0, i)),
            pl.BlockSpec((4, chunk), lambda i: (0, i)),
            pl.BlockSpec((VIEWS_DEV, 2, chunk), lambda i: (0, 0, i)),
            pl.BlockSpec((VIEWS_DEV, chunk), lambda i: (0, i)),
        ],
        out_specs=pl.BlockSpec((2, BLOCKS // 4, LANES), lambda i: (0, i, 0)),
        out_shape=VMEM((2, BLOCKS, LANES), f32),
        scratch_shapes=[pltpu.VMEM((216, LANES), f32)],
        compiler_params=LIMIT,
        name="views",
    )(rotation, shift, focal, means, scales, quats, grad_screen, visible)
    other = lax.ppermute(squares, "view", [(v, v ^ 1) for v in range(8)])
    squares = [jnp.maximum(squares, other)]
    for k in (1, 2, 3):
        pairs = [(v, (v + 2 * k) % 8) for v in range(8)]
        squares.append(lax.ppermute(squares[0], "view", pairs))

    start, index = pl.pallas_call(
        index_kernel,
        in_specs=[vmem()],
        out_specs=[vmem()] * 2,
        out_shape=[
            VMEM((8, LANES), i32),
            VMEM((BLOCKS, LANES), i32),
        ],
        compiler_params=LIMIT,
        name="index",
    )(mask)
    filled, total, branch = pl.pallas_call(
        fill_kernel,
        grid_spec=pltpu.PrefetchScalarGridSpec(
            num_scalar_prefetch=1,
            grid=(1,),
            in_specs=[
                smem(),
                smem(),
                whole(BLOCKS, LANES),
                whole(3, G_DEV),
                whole(3, G_DEV),
                whole(4, G_DEV),
                pl.BlockSpec((8, G_DEV), lambda i, w: (jnp.maximum(w[0] - 2, 0), 0)),
                pl.BlockSpec((8, G_DEV), lambda i, w: (jnp.maximum(w[0] - 1, 0), 0)),
            ],
            out_specs=[whole(BLOCKS, 8, LANES), smem(), smem()],
            scratch_shapes=[pltpu.VMEM((8, G_DEV), f32)],
        ),
        out_shape=[
            VMEM((BLOCKS, 8, LANES), f32),
            jax.ShapeDtypeStruct((1,), i32),
            jax.ShapeDtypeStruct((1,), i32),
        ],
        compiler_params=LIMIT,
        name="fill",
    )(where, counts, start, index, means, scales, quats, attrs, attrs)
    outgoing, peak = pl.pallas_call(
        peak_kernel,
        in_specs=[smem()] * 3 + [vmem()] * 6,
        out_specs=[vmem()] * 2,
        out_shape=[
            VMEM((BLOCKS, 8, LANES), f32),
            jax.ShapeDtypeStruct((2, G_DEV), f32),
        ],
        scratch_shapes=[pltpu.VMEM((2 * BLOCKS + 32, LANES), f32)],
        compiler_params=LIMIT,
        name="peaks",
    )(where, counts, start, index, *squares, filled)

    def gather(cap):
        def go(where, counts, outgoing):
            arrived = lax.all_to_all(
                outgoing.reshape(SHARDS, PER, 8, LANES), "gauss", 0, 0, tiled=True
            ).reshape(BLOCKS, 8, LANES)
            piece = pl.pallas_call(
                place_kernel,
                in_specs=[smem(), smem(), vmem()],
                out_specs=vmem(),
                out_shape=VMEM((4, cap, 8, LANES), f32),
                scratch_shapes=[pltpu.VMEM((cap + 1, 8, LANES), f32)],
                compiler_params=LIMIT,
                name="place",
            )(where, counts, arrived)
            cores = [[0, 2, 4, 6], [1, 3, 5, 7]]
            own = lax.all_to_all(piece, "view", 0, 0, axis_index_groups=cores, tiled=True)
            other = lax.ppermute(own, "view", [(v, v ^ 1) for v in range(8)])
            return pl.pallas_call(
                join_kernel,
                in_specs=[smem(), vmem(), vmem()],
                out_specs=pl.BlockSpec(memory_space=pl.ANY),
                out_shape=jax.ShapeDtypeStruct((ROWS, G_DEV), f32),
                scratch_shapes=[pltpu.VMEM((8, 8, G_DEV), f32), pltpu.SemaphoreType.DMA((8,))],
                compiler_params=LIMIT,
                name="join",
            )(where, own, other)

        return go

    clones = lax.switch(
        branch[0],
        [gather(cap) for cap in range(STEP, BLOCKS + 1, STEP)],
        where,
        counts,
        outgoing,
    )
    return (peak, clones, total[0])


def solution(mesh):
    return jax.shard_map(
        body,
        mesh=mesh,
        in_specs=(
            P(None, "gauss"),
            P(None, "gauss"),
            P(None, "gauss"),
            P(None, "gauss"),
            P("view", None, "gauss"),
            P("view", "gauss"),
            P("gauss"),
            P("view", None, None),
            P("view", None),
            P("view"),
        ),
        out_specs=(P(None, "gauss"), P(None, "gauss"), P()),
        check_vma=False,
    )
```

```python
import jax
import jax.numpy as jnp
from jax import lax
from jax.experimental import pallas as pl
from jax.experimental.pallas import tpu as pltpu
from jax.sharding import PartitionSpec as P

G_DEV = 16384
LANES = 128
BLOCKS = G_DEV // LANES
SHARDS = 32
PER = BLOCKS // SHARDS
VIEWS_DEV = 4
CAPS = (16, 32, 40, 48, 56, 64, 80, 96, BLOCKS)
ROWS = 61
LIMIT = pltpu.CompilerParams(vmem_limit_bytes=16 * 2**20)
SMEM = pltpu.MemorySpace.SMEM
VMEM = pltpu.MemorySpace.VMEM


def dot(a, b, dims=((1,), (0,))):
    return lax.dot_general(a, b, (dims, ((), ())), preferred_element_type=jnp.float32)


def where_1(cond):
    return jnp.where(cond, 1.0, 0.0).astype(jnp.bfloat16)


def count_kernel(mask_ref, count_ref):
    total = jnp.sum(jnp.sum(mask_ref[...], axis=0, keepdims=True), axis=1, keepdims=True)
    count_ref[...] = jnp.broadcast_to(total, (SHARDS, LANES))


def index_kernel(mask_ref, start_ref, index_ref):
    marked = mask_ref[...]
    ones = marked.astype(jnp.float32).astype(jnp.bfloat16)
    row = lax.broadcasted_iota(jnp.int32, (LANES, LANES), 0)
    lane = lax.broadcasted_iota(jnp.int32, (LANES, LANES), 1)
    full = jnp.ones((LANES, LANES), jnp.bfloat16)

    inclusive = dot(ones, where_1(row <= lane)).astype(jnp.int32)
    in_row = dot(ones, full)
    start = dot(where_1(row > lane), in_row.astype(jnp.bfloat16)).astype(jnp.int32)
    in_row_t = dot(jnp.ones((8, LANES), jnp.bfloat16), ones, ((1,), (1,)))
    start_ref[...] = dot(in_row_t.astype(jnp.bfloat16), where_1(row < lane)).astype(jnp.int32)

    moves = lane - inclusive + 1
    code = jnp.where(marked == 1, moves * 256 + lane, 0)
    for bit in range(7):
        moved = pltpu.roll(code, LANES - (1 << bit), 1)
        take = ((moved >> (8 + bit)) & 1) == 1
        leave = ((code >> (8 + bit)) & 1) == 1
        code = jnp.where(take, moved, jnp.where(leave, 0, code))
    first = start & (LANES - 1)
    nth = (lane - first) & (LANES - 1)
    source = jnp.take_along_axis(
        code & (LANES - 1), nth, axis=1, mode="promise_in_bounds"
    )
    valid = nth < in_row.astype(jnp.int32)
    here = jnp.where(valid, jnp.where(lane >= first, 256, 512), 0)
    index_ref[...] = source + here


def view_kernel(rot, trans, focal, means, scales, quats, grad, seen, out_ref, scr):
    width = 23

    def group(g, carry):
        for j in range(8):
            col = pl.ds(pl.multiple_of(g * 1024 + j * LANES, LANES), LANES)
            base = j * width
            scr[base : base + 3, :] = means[:, col]
            scr[base + 3 : base + 6, :] = scales[:, col]
            scr[base + 6 : base + 10, :] = quats[:, col]
            for v in range(VIEWS_DEV):
                scr[base + 10 + 2 * v : base + 12 + 2 * v, :] = grad[v, :, col]
            scr[base + 18 : base + 22, :] = seen[:, col].astype(jnp.float32)

        def comp(r):
            return scr[pl.ds(r, 8, stride=width), :]

        m = [comp(i) for i in range(3)]
        sc = [comp(3 + i) for i in range(3)]
        q = [comp(6 + i) for i in range(4)]
        norm = q[0] * q[0] + q[1] * q[1] + q[2] * q[2] + q[3] * q[3]
        inv = 1.0 / jnp.sqrt(norm + 0.25)
        w, x, y, z = (c * inv for c in q)
        rq = [
            [1 - 2 * (y * y + z * z), 2 * (x * y - w * z), 2 * (x * z + w * y)],
            [2 * (x * y + w * z), 1 - 2 * (x * x + z * z), 2 * (y * z - w * x)],
            [2 * (x * z - w * y), 2 * (y * z + w * x), 1 - 2 * (x * x + y * y)],
        ]
        factor = [[rq[i][j] * sc[j] for j in range(3)] for i in range(3)]
        gmax = jnp.zeros((8, LANES), jnp.float32)
        lmax = jnp.zeros((8, LANES), jnp.float32)
        for v in range(VIEWS_DEV):
            r = [[rot[i, v, j] for j in range(3)] for i in range(3)]
            f = focal[0, v]
            p = [r[i][0] * m[0] + r[i][1] * m[1] + r[i][2] * m[2] + trans[v, i] for i in range(3)]
            over = 1.0 / jnp.maximum(p[2], 1.0)
            j00 = f * over
            j02 = -(j00 * p[0]) * over
            j12 = -(j00 * p[1]) * over
            first = [j00 * r[0][j] + j02 * r[2][j] for j in range(3)]
            second = [j00 * r[1][j] + j12 * r[2][j] for j in range(3)]
            pr = [sum(first[j] * factor[j][k] for j in range(3)) for k in range(3)]
            qr = [sum(second[j] * factor[j][k] for j in range(3)) for k in range(3)]
            a = pr[0] * pr[0] + pr[1] * pr[1] + pr[2] * pr[2] + 0.3
            c = qr[0] * qr[0] + qr[1] * qr[1] + qr[2] * qr[2] + 0.3
            b = pr[0] * qr[0] + pr[1] * qr[1] + pr[2] * qr[2]
            half = 0.5 * (a - c)
            lam = 0.5 * (a + c) + jnp.sqrt(half * half + b * b + 0.01)
            vis = comp(18 + v)
            g0 = comp(10 + 2 * v)
            g1 = comp(11 + 2 * v)
            gmax = jnp.maximum(gmax, (g0 * g0 + g1 * g1) * vis)
            lmax = jnp.maximum(lmax, lam * vis)
        rows = pl.ds(pl.multiple_of(g * 8, 8), 8)
        out_ref[0, rows, :] = gmax
        out_ref[1, rows, :] = lmax
        return carry

    lax.fori_loop(0, means.shape[1] // 1024, group, 0)


def blocks_before(counts, upto):
    total = jnp.int32(0)
    for t in range(SHARDS):
        total = total + jnp.where(t < upto, (counts[t, 0] + LANES - 1) // LANES, 0)
    return total


def each_block(where, counts, start, index, rows, store):
    offset = blocks_before(counts, where[1])

    def place_of(block):
        return ((offset + block) & (SHARDS - 1)) * PER + (block >> 5)

    def eight(i, carry):
        for j in range(8):
            b = i * 8 + j
            block = start[0, b] >> 7
            code = jnp.broadcast_to(index[pl.ds(b, 1), :], (8, LANES))
            tile = rows[:, pl.ds(pl.multiple_of(b * LANES, LANES), LANES)]
            packed = jnp.take_along_axis(
                tile, code & (LANES - 1), axis=1, mode="promise_in_bounds"
            )
            store(place_of(block), packed, (code & 256) != 0)
            after = jnp.minimum(block + 1, BLOCKS - 1)
            store(place_of(after), packed, (code & 512) != 0)
        return carry

    lax.fori_loop(0, BLOCKS // 8, eight, 0)


def fill_kernel(
    where, counts, start, index, means, scales, quats, low, high, out_ref, sums_ref, pick_ref, rows
):
    view = where[0]

    @pl.when(view == 0)
    def _():
        rows[0:3, :] = means[...]
        rows[3:6, :] = scales[...]
        rows[6:8, :] = quats[0:2, :]

    @pl.when(view == 1)
    def _():
        rows[0:2, :] = quats[2:4, :]

    @pl.when(view > 1)
    def _():
        rows[0:2, :] = low[6:8, :]

    @pl.when((view > 0) & (view < 7))
    def _():
        rows[2:8, :] = high[0:6, :]

    @pl.when(view == 7)
    def _():
        rows[2:3, :] = high[0:1, :]
        rows[3:8, :] = jnp.zeros((5, G_DEV), jnp.float32)

    total = jnp.int32(0)
    for t in range(SHARDS):
        total = total + counts[t, 0]
    sums_ref[0] = total
    used = blocks_before(counts, SHARDS)
    pick = jnp.int32(0)
    for cap in CAPS[:-1]:
        pick = pick + jnp.where(used > cap * SHARDS, 1, 0)
    pick_ref[0] = pick

    zero = jnp.zeros((8, LANES), jnp.float32)
    for i in range(BLOCKS):
        out_ref[i] = zero

    def store(at, packed, mask):
        pltpu.store(out_ref.at[at], packed, mask=mask)

    each_block(where, counts, start, index, rows, store)


def top_of(squares, k, at):
    a, b, c, d = (sq[k, at, :] for sq in squares)
    return jnp.maximum(jnp.maximum(a, b), jnp.maximum(c, d))


def add_kernel(where, counts, start, index, sq0, sq1, sq2, sq3, filled, out_ref, pairs):
    @pl.when(where[0] == 7)
    def _():
        offset = blocks_before(counts, where[1])

        def place_of(block):
            return ((offset + block) & (SHARDS - 1)) * PER + (block >> 5)

        for g in range(BLOCKS // 8):
            at = slice(8 * g, 8 * g + 8)
            lanes = index[at, :] & (LANES - 1)
            for k in range(2):
                root = jnp.sqrt(top_of((sq0, sq1, sq2, sq3), k, at))
                pairs[pl.ds(16 * g + k, 8, stride=2), :] = jnp.take_along_axis(
                    root if k == 0 else 3.0 * root, lanes, axis=1, mode="promise_in_bounds"
                )
        for b in range(BLOCKS):
            block = start[0, b] >> 7
            after = jnp.minimum(block + 1, BLOCKS - 1)
            code = jnp.broadcast_to(index[b : b + 1, :], (2, LANES))
            two = pairs[2 * b : 2 * b + 2, :]
            pltpu.store(out_ref.at[place_of(block), 3:5, :], two, mask=(code & 256) != 0)
            pltpu.store(out_ref.at[place_of(after), 3:5, :], two, mask=(code & 512) != 0)


def peak_kernel(sq0, sq1, sq2, sq3, peak_ref, pairs):
    for g in range(BLOCKS // 8):
        at = slice(8 * g, 8 * g + 8)
        norm = jnp.sqrt(top_of((sq0, sq1, sq2, sq3), 0, at))
        radius = 3.0 * jnp.sqrt(top_of((sq0, sq1, sq2, sq3), 1, at))
        pairs[pl.ds(16 * g, 8, stride=2), :] = norm
        pairs[pl.ds(16 * g + 1, 8, stride=2), :] = radius
    for b in range(BLOCKS):
        peak_ref[:, b * LANES : (b + 1) * LANES] = pairs[2 * b : 2 * b + 2, :]


def place_kernel(where, counts, arrived, out_ref, slots):
    cap = out_ref.shape[1]
    mine = where[1]
    zero = jnp.zeros((8, LANES), jnp.float32)
    for i in range(cap):
        slots[i] = zero
    before = jnp.int32(0)
    for s in range(SHARDS):
        local = (mine - before) & (SHARDS - 1)
        first = (before + local) >> 5
        for w in range(PER):
            slots[jnp.minimum(first + w, cap)] = arrived[s * PER + w]
        before = before + (counts[s, 0] + LANES - 1) // LANES
    for i in range(cap):
        tile = slots[i]
        for x in range(4):
            out_ref[x, i] = tile


def row_copy(buf, out_ref, sems, r, columns):
    rows = min(8, ROWS - 8 * r)
    return pltpu.make_async_copy(
        buf.at[r, 0:rows, columns], out_ref.at[8 * r : 8 * r + rows, columns], sems.at[r]
    )


def own_kernel(where, own, out_ref, buf, sems):
    cap = own.shape[1]
    core = where[0] & 1
    empty = slice(cap * LANES, G_DEV)
    for half in range(2):

        @pl.when(core == half)
        def _():
            for r in range(8):
                for i in range(cap, BLOCKS):
                    buf[r, :, i * LANES : (i + 1) * LANES] = jnp.zeros((8, LANES), jnp.float32)
                if r % 2 == half:
                    for i in range(cap):
                        buf[r, :, i * LANES : (i + 1) * LANES] = own[r // 2, i]
                    row_copy(buf, out_ref, sems, r, slice(0, G_DEV)).start()
                elif cap < BLOCKS:
                    row_copy(buf, out_ref, sems, r, empty).start()
            for r in range(8):
                if r % 2 == half:
                    row_copy(buf, out_ref, sems, r, slice(0, G_DEV)).wait()
                elif cap < BLOCKS:
                    row_copy(buf, out_ref, sems, r, empty).wait()


def other_kernel(where, other, begun, out_ref, buf, sems):
    cap = other.shape[1]
    core = where[0] & 1
    for half in range(2):

        @pl.when(core == half)
        def _():
            for r in range(1 - half, 8, 2):
                for i in range(cap):
                    buf[r, :, i * LANES : (i + 1) * LANES] = other[r // 2, i]
                row_copy(buf, out_ref, sems, r, slice(0, cap * LANES)).start()
            for r in range(1 - half, 8, 2):
                row_copy(buf, out_ref, sems, r, slice(0, cap * LANES)).wait()


def smem():
    return pl.BlockSpec(memory_space=SMEM)


def vmem():
    return pl.BlockSpec(memory_space=VMEM)


def body(means, scales, quats, attrs, grad_screen, visible, clone_mask, rotation, shift, focal):
    f32, i32 = jnp.float32, jnp.int32
    view = lax.axis_index("view")
    where = jnp.stack([view, lax.axis_index("gauss")]).astype(i32)

    def whole(*shape):
        return pl.BlockSpec(shape, lambda i, w: (0,) * len(shape))

    mask = clone_mask.reshape(BLOCKS, LANES)
    rotation, focal = rotation.transpose(1, 0, 2), focal.reshape(1, VIEWS_DEV)
    mask, means, scales, quats, attrs, grad_screen, visible, rotation, shift, focal = (
        pltpu.with_memory_space_constraint(x, pltpu.MemorySpace.HBM)
        for x in (
            mask, means, scales, quats, attrs, grad_screen, visible, rotation, shift, focal
        )
    )
    count = pl.pallas_call(
        count_kernel,
        in_specs=[vmem()],
        out_specs=vmem(),
        out_shape=VMEM((SHARDS, LANES), i32),
        compiler_params=LIMIT,
        name="count",
    )(mask)
    counts = lax.all_to_all(count, "gauss", 0, 0, tiled=True)

    squares = pl.pallas_call(
        view_kernel,
        in_specs=[smem()] * 3 + [vmem()] * 5,
        out_specs=vmem(),
        out_shape=VMEM((2, BLOCKS, LANES), f32),
        scratch_shapes=[pltpu.VMEM((216, LANES), f32)],
        compiler_params=LIMIT,
        name="views",
    )(rotation, shift, focal, means, scales, quats, grad_screen, visible)
    other = lax.ppermute(squares, "view", [(v, v ^ 1) for v in range(8)])
    squares = [jnp.maximum(squares, other)]
    for k in (1, 2, 3):
        pairs = [(v, (v + 2 * k) % 8) for v in range(8)]
        squares.append(lax.ppermute(squares[0], "view", pairs))

    start, index = pl.pallas_call(
        index_kernel,
        in_specs=[vmem()],
        out_specs=[vmem()] * 2,
        out_shape=[
            VMEM((8, LANES), i32),
            VMEM((BLOCKS, LANES), i32),
        ],
        compiler_params=LIMIT,
        name="index",
    )(mask)
    filled, total, branch = pl.pallas_call(
        fill_kernel,
        grid_spec=pltpu.PrefetchScalarGridSpec(
            num_scalar_prefetch=1,
            grid=(1,),
            in_specs=[
                smem(),
                smem(),
                whole(BLOCKS, LANES),
                whole(3, G_DEV),
                whole(3, G_DEV),
                whole(4, G_DEV),
                pl.BlockSpec((8, G_DEV), lambda i, w: (jnp.maximum(w[0] - 2, 0), 0)),
                pl.BlockSpec((8, G_DEV), lambda i, w: (jnp.maximum(w[0] - 1, 0), 0)),
            ],
            out_specs=[whole(BLOCKS, 8, LANES), smem(), smem()],
            scratch_shapes=[pltpu.VMEM((8, G_DEV), f32)],
        ),
        out_shape=[
            VMEM((BLOCKS, 8, LANES), f32),
            jax.ShapeDtypeStruct((1,), i32),
            jax.ShapeDtypeStruct((1,), i32),
        ],
        compiler_params=LIMIT,
        name="fill",
    )(where, counts, start, index, means, scales, quats, attrs, attrs)
    outgoing = pl.pallas_call(
        add_kernel,
        in_specs=[smem()] * 3 + [vmem()] * 6,
        out_specs=vmem(),
        out_shape=VMEM((BLOCKS, 8, LANES), f32),
        input_output_aliases={8: 0},
        scratch_shapes=[pltpu.VMEM((2 * BLOCKS + 32, LANES), f32)],
        compiler_params=LIMIT,
        name="add",
    )(where, counts, start, index, *squares, filled)

    def gather(cap):
        def go(where, counts, outgoing, *squares):
            arrived = lax.all_to_all(
                outgoing.reshape(SHARDS, PER, 8, LANES), "gauss", 0, 0, tiled=True
            ).reshape(BLOCKS, 8, LANES)
            piece = pl.pallas_call(
                place_kernel,
                in_specs=[smem(), smem(), vmem()],
                out_specs=vmem(),
                out_shape=VMEM((4, cap, 8, LANES), f32),
                scratch_shapes=[pltpu.VMEM((cap + 1, 8, LANES), f32)],
                compiler_params=LIMIT,
                name="place",
            )(where, counts, arrived)
            cores = [[0, 2, 4, 6], [1, 3, 5, 7]]
            own = lax.all_to_all(piece, "view", 0, 0, axis_index_groups=cores, tiled=True)
            other = lax.ppermute(own, "view", [(v, v ^ 1) for v in range(8)])
            peak = pl.pallas_call(
                peak_kernel,
                in_specs=[vmem()] * 4,
                out_specs=vmem(),
                out_shape=pltpu.MemorySpace.HBM((2, G_DEV), f32),
                scratch_shapes=[pltpu.VMEM((2 * BLOCKS + 32, LANES), f32)],
                compiler_params=LIMIT,
                name="peaks",
            )(*squares)
            begun = pl.pallas_call(
                own_kernel,
                in_specs=[smem(), vmem()],
                out_specs=pl.BlockSpec(memory_space=pl.ANY),
                out_shape=jax.ShapeDtypeStruct((ROWS, G_DEV), f32),
                scratch_shapes=[pltpu.VMEM((8, 8, G_DEV), f32), pltpu.SemaphoreType.DMA((8,))],
                compiler_params=LIMIT,
                name="own",
            )(where, own)
            clones = pl.pallas_call(
                other_kernel,
                in_specs=[smem(), vmem(), pl.BlockSpec(memory_space=pl.ANY)],
                out_specs=pl.BlockSpec(memory_space=pl.ANY),
                out_shape=jax.ShapeDtypeStruct((ROWS, G_DEV), f32),
                input_output_aliases={2: 0},
                scratch_shapes=[pltpu.VMEM((8, 8, G_DEV), f32), pltpu.SemaphoreType.DMA((8,))],
                compiler_params=LIMIT,
                name="other",
            )(where, other, begun)
            return peak, clones

        return go

    peak, clones = lax.switch(
        branch[0], [gather(cap) for cap in CAPS], where, counts, outgoing, *squares
    )
    return (peak, clones, total[0])


def solution(mesh):
    return jax.shard_map(
        body,
        mesh=mesh,
        in_specs=(
            P(None, "gauss"),
            P(None, "gauss"),
            P(None, "gauss"),
            P(None, "gauss"),
            P("view", None, "gauss"),
            P("view", "gauss"),
            P("gauss"),
            P("view", None, None),
            P("view", None),
            P("view"),
        ),
        out_specs=(P(None, "gauss"), P(None, "gauss"), P()),
        check_vma=False,
    )
```

```python
import jax
import jax.numpy as jnp
from jax import lax
from jax.experimental import pallas as pl
from jax.experimental.pallas import tpu as pltpu
from jax.sharding import PartitionSpec as P

G_DEV = 16384
LANES = 128
BLOCKS = G_DEV // LANES
SHARDS = 32
PER = BLOCKS // SHARDS
VIEWS_DEV = 4
CAPS = (16, 32, 40, 48, 56, 64, 80, 96, BLOCKS)
ROWS = 61
LIMIT = pltpu.CompilerParams(vmem_limit_bytes=16 * 2**20)
SMEM = pltpu.MemorySpace.SMEM
VMEM = pltpu.MemorySpace.VMEM


def dot(a, b, dims=((1,), (0,))):
    return lax.dot_general(a, b, (dims, ((), ())), preferred_element_type=jnp.float32)


def where_1(cond):
    return jnp.where(cond, 1.0, 0.0).astype(jnp.bfloat16)


def count_kernel(mask_ref, count_ref):
    total = jnp.sum(jnp.sum(mask_ref[...], axis=0, keepdims=True), axis=1, keepdims=True)
    count_ref[...] = jnp.broadcast_to(total, (SHARDS, LANES))


def index_kernel(mask_ref, start_ref, index_ref):
    marked = mask_ref[...]
    ones = marked.astype(jnp.float32).astype(jnp.bfloat16)
    row = lax.broadcasted_iota(jnp.int32, (LANES, LANES), 0)
    lane = lax.broadcasted_iota(jnp.int32, (LANES, LANES), 1)
    full = jnp.ones((LANES, LANES), jnp.bfloat16)

    inclusive = dot(ones, where_1(row <= lane)).astype(jnp.int32)
    in_row = dot(ones, full)
    start = dot(where_1(row > lane), in_row.astype(jnp.bfloat16)).astype(jnp.int32)
    in_row_t = dot(jnp.ones((8, LANES), jnp.bfloat16), ones, ((1,), (1,)))
    start_ref[...] = dot(in_row_t.astype(jnp.bfloat16), where_1(row < lane)).astype(jnp.int32)

    moves = lane - inclusive + 1
    code = jnp.where(marked == 1, moves * 256 + lane, 0)
    for bit in range(7):
        moved = pltpu.roll(code, LANES - (1 << bit), 1)
        take = ((moved >> (8 + bit)) & 1) == 1
        leave = ((code >> (8 + bit)) & 1) == 1
        code = jnp.where(take, moved, jnp.where(leave, 0, code))
    first = start & (LANES - 1)
    nth = (lane - first) & (LANES - 1)
    source = jnp.take_along_axis(
        code & (LANES - 1), nth, axis=1, mode="promise_in_bounds"
    )
    valid = nth < in_row.astype(jnp.int32)
    here = jnp.where(valid, jnp.where(lane >= first, 256, 512), 0)
    index_ref[...] = source + here


def view_kernel(rot, trans, focal, means, scales, quats, grad, seen, out_ref, scr):
    width = 23

    def group(g, carry):
        for j in range(8):
            col = pl.ds(pl.multiple_of(g * 1024 + j * LANES, LANES), LANES)
            base = j * width
            scr[base : base + 3, :] = means[:, col]
            scr[base + 3 : base + 6, :] = scales[:, col]
            scr[base + 6 : base + 10, :] = quats[:, col]
            for v in range(VIEWS_DEV):
                scr[base + 10 + 2 * v : base + 12 + 2 * v, :] = grad[v, :, col]
            scr[base + 18 : base + 22, :] = seen[:, col].astype(jnp.float32)

        def comp(r):
            return scr[pl.ds(r, 8, stride=width), :]

        m = [comp(i) for i in range(3)]
        sc = [comp(3 + i) for i in range(3)]
        q = [comp(6 + i) for i in range(4)]
        norm = q[0] * q[0] + q[1] * q[1] + q[2] * q[2] + q[3] * q[3]
        inv = 1.0 / jnp.sqrt(norm + 0.25)
        w, x, y, z = (c * inv for c in q)
        rq = [
            [1 - 2 * (y * y + z * z), 2 * (x * y - w * z), 2 * (x * z + w * y)],
            [2 * (x * y + w * z), 1 - 2 * (x * x + z * z), 2 * (y * z - w * x)],
            [2 * (x * z - w * y), 2 * (y * z + w * x), 1 - 2 * (x * x + y * y)],
        ]
        factor = [[rq[i][j] * sc[j] for j in range(3)] for i in range(3)]
        gmax = jnp.zeros((8, LANES), jnp.float32)
        lmax = jnp.zeros((8, LANES), jnp.float32)
        for v in range(VIEWS_DEV):
            r = [[rot[i, v, j] for j in range(3)] for i in range(3)]
            f = focal[0, v]
            p = [r[i][0] * m[0] + r[i][1] * m[1] + r[i][2] * m[2] + trans[v, i] for i in range(3)]
            over = 1.0 / jnp.maximum(p[2], 1.0)
            j00 = f * over
            j02 = -(j00 * p[0]) * over
            j12 = -(j00 * p[1]) * over
            first = [j00 * r[0][j] + j02 * r[2][j] for j in range(3)]
            second = [j00 * r[1][j] + j12 * r[2][j] for j in range(3)]
            pr = [sum(first[j] * factor[j][k] for j in range(3)) for k in range(3)]
            qr = [sum(second[j] * factor[j][k] for j in range(3)) for k in range(3)]
            a = pr[0] * pr[0] + pr[1] * pr[1] + pr[2] * pr[2] + 0.3
            c = qr[0] * qr[0] + qr[1] * qr[1] + qr[2] * qr[2] + 0.3
            b = pr[0] * qr[0] + pr[1] * qr[1] + pr[2] * qr[2]
            half = 0.5 * (a - c)
            lam = 0.5 * (a + c) + jnp.sqrt(half * half + b * b + 0.01)
            vis = comp(18 + v)
            g0 = comp(10 + 2 * v)
            g1 = comp(11 + 2 * v)
            gmax = jnp.maximum(gmax, (g0 * g0 + g1 * g1) * vis)
            lmax = jnp.maximum(lmax, lam * vis)
        rows = pl.ds(pl.multiple_of(g * 8, 8), 8)
        out_ref[0, rows, :] = gmax
        out_ref[1, rows, :] = lmax
        return carry

    lax.fori_loop(0, means.shape[1] // 1024, group, 0)


def fill_kernel(
    where, counts, start, index, means, scales, quats, low, high,
    out_ref, sums_ref, pick_ref, table, rows
):
    view = where[0]

    @pl.when(view == 0)
    def _():
        rows[0:3, :] = means[...]
        rows[3:6, :] = scales[...]
        rows[6:8, :] = quats[0:2, :]

    @pl.when(view == 1)
    def _():
        rows[0:2, :] = quats[2:4, :]

    @pl.when(view > 1)
    def _():
        rows[0:2, :] = low[6:8, :]

    @pl.when((view > 0) & (view < 7))
    def _():
        rows[2:8, :] = high[0:6, :]

    @pl.when(view == 7)
    def _():
        rows[2:3, :] = high[0:1, :]
        rows[3:8, :] = jnp.zeros((5, G_DEV), jnp.float32)

    zero = jnp.zeros((8, LANES), jnp.float32)
    for i in range(BLOCKS):
        out_ref[i] = zero

    mine = where[1]
    total = offset = used = jnp.int32(0)
    for s in range(SHARDS):
        offset = jnp.where(s == mine, used, offset)
        local = (mine - used) & (SHARDS - 1)
        first = (used + local) >> 5
        for w in range(PER):
            table[BLOCKS + s * PER + w] = first + w
        count = counts[s, 0]
        total = total + count
        used = used + ((count + LANES - 1) >> 7)
    sums_ref[0] = total
    pick = jnp.int32(0)
    for cap in CAPS[:-1]:
        pick = pick + jnp.where(used > cap * SHARDS, 1, 0)
    pick_ref[0] = pick
    table[2 * BLOCKS] = view

    def place_of(block):
        return ((offset + block) & (SHARDS - 1)) * PER + (block >> 5)

    def eight(i, carry):
        for j in range(8):
            b = i * 8 + j
            block = start[0, b] >> 7
            here = place_of(block)
            after = place_of(jnp.minimum(block + 1, BLOCKS - 1))
            table[b] = here + (after << 8)
            code = jnp.broadcast_to(index[pl.ds(b, 1), :], (8, LANES))
            tile = rows[:, pl.ds(pl.multiple_of(b * LANES, LANES), LANES)]
            packed = jnp.take_along_axis(
                tile, code & (LANES - 1), axis=1, mode="promise_in_bounds"
            )
            pltpu.store(out_ref.at[here], packed, mask=(code & 256) != 0)
            pltpu.store(out_ref.at[after], packed, mask=(code & 512) != 0)
        return carry

    lax.fori_loop(0, BLOCKS // 8, eight, 0)


def top_of(squares, k, at):
    a, b, c, d = (sq[k, at, :] for sq in squares)
    return jnp.maximum(jnp.maximum(a, b), jnp.maximum(c, d))


def add_kernel(table, index, sq0, sq1, sq2, sq3, filled, out_ref, pairs):
    @pl.when(table[2 * BLOCKS] == 7)
    def _():
        for g in range(BLOCKS // 8):
            at = slice(8 * g, 8 * g + 8)
            lanes = index[at, :] & (LANES - 1)
            for k in range(2):
                root = jnp.sqrt(top_of((sq0, sq1, sq2, sq3), k, at))
                pairs[pl.ds(16 * g + k, 8, stride=2), :] = jnp.take_along_axis(
                    root if k == 0 else 3.0 * root, lanes, axis=1, mode="promise_in_bounds"
                )
        for b in range(BLOCKS):
            both = table[b]
            code = jnp.broadcast_to(index[b : b + 1, :], (2, LANES))
            two = pairs[2 * b : 2 * b + 2, :]
            pltpu.store(out_ref.at[both & 255, 3:5, :], two, mask=(code & 256) != 0)
            pltpu.store(out_ref.at[both >> 8, 3:5, :], two, mask=(code & 512) != 0)


def peak_kernel(sq0, sq1, sq2, sq3, peak_ref, pairs):
    for g in range(BLOCKS // 8):
        at = slice(8 * g, 8 * g + 8)
        norm = jnp.sqrt(top_of((sq0, sq1, sq2, sq3), 0, at))
        radius = 3.0 * jnp.sqrt(top_of((sq0, sq1, sq2, sq3), 1, at))
        pairs[pl.ds(16 * g, 8, stride=2), :] = norm
        pairs[pl.ds(16 * g + 1, 8, stride=2), :] = radius
    for b in range(BLOCKS):
        peak_ref[:, b * LANES : (b + 1) * LANES] = pairs[2 * b : 2 * b + 2, :]


def place_kernel(table, arrived, out_ref, slots):
    cap = out_ref.shape[1]
    zero = jnp.zeros((8, LANES), jnp.float32)
    for i in range(cap):
        slots[i] = zero
    for i in range(BLOCKS):
        slots[jnp.minimum(table[BLOCKS + i], cap)] = arrived[i]
    for i in range(cap):
        tile = slots[i]
        for x in range(4):
            out_ref[x, i] = tile


def row_copy(buf, out_ref, sems, r, columns):
    rows = min(8, ROWS - 8 * r)
    return pltpu.make_async_copy(
        buf.at[r, 0:rows, columns], out_ref.at[8 * r : 8 * r + rows, columns], sems.at[r]
    )


def own_kernel(where, own, out_ref, buf, zeros, sems):
    cap = own.shape[1]
    core = where[0] & 1

    def clear(r):
        rows = min(8, ROWS - 8 * r)
        return pltpu.make_async_copy(
            zeros.at[0:rows, :],
            out_ref.at[8 * r : 8 * r + rows, cap * LANES : G_DEV],
            sems.at[8 + r],
        )

    if cap < BLOCKS:
        for i in range(BLOCKS - cap):
            zeros[:, i * LANES : (i + 1) * LANES] = jnp.zeros((8, LANES), jnp.float32)
        for r in range(8):
            clear(r).start()
    for half in range(2):

        @pl.when(core == half)
        def _():
            for r in range(half, 8, 2):
                for i in range(cap):
                    buf[r, :, i * LANES : (i + 1) * LANES] = own[r // 2, i]
                row_copy(buf, out_ref, sems, r, slice(0, cap * LANES)).start()
            for r in range(half, 8, 2):
                row_copy(buf, out_ref, sems, r, slice(0, cap * LANES)).wait()

    if cap < BLOCKS:
        for r in range(8):
            clear(r).wait()


def other_kernel(where, other, begun, out_ref, buf, sems):
    cap = other.shape[1]
    core = where[0] & 1
    for half in range(2):

        @pl.when(core == half)
        def _():
            for r in range(1 - half, 8, 2):
                for i in range(cap):
                    buf[r, :, i * LANES : (i + 1) * LANES] = other[r // 2, i]
                row_copy(buf, out_ref, sems, r, slice(0, cap * LANES)).start()
            for r in range(1 - half, 8, 2):
                row_copy(buf, out_ref, sems, r, slice(0, cap * LANES)).wait()


def smem():
    return pl.BlockSpec(memory_space=SMEM)


def vmem():
    return pl.BlockSpec(memory_space=VMEM)


def body(means, scales, quats, attrs, grad_screen, visible, clone_mask, rotation, shift, focal):
    f32, i32 = jnp.float32, jnp.int32
    view = lax.axis_index("view")
    where = jnp.stack([view, lax.axis_index("gauss")]).astype(i32)

    def whole(*shape):
        return pl.BlockSpec(shape, lambda i, w: (0,) * len(shape))

    mask = clone_mask.reshape(BLOCKS, LANES)
    rotation, focal = rotation.transpose(1, 0, 2), focal.reshape(1, VIEWS_DEV)
    mask, means, scales, quats, attrs, grad_screen, visible, rotation, shift, focal = (
        pltpu.with_memory_space_constraint(x, pltpu.MemorySpace.HBM)
        for x in (
            mask, means, scales, quats, attrs, grad_screen, visible, rotation, shift, focal
        )
    )
    count = pl.pallas_call(
        count_kernel,
        in_specs=[vmem()],
        out_specs=vmem(),
        out_shape=VMEM((SHARDS, LANES), i32),
        compiler_params=LIMIT,
        name="count",
    )(mask)
    counts = lax.all_to_all(count, "gauss", 0, 0, tiled=True)

    squares = pl.pallas_call(
        view_kernel,
        in_specs=[smem()] * 3 + [vmem()] * 5,
        out_specs=vmem(),
        out_shape=VMEM((2, BLOCKS, LANES), f32),
        scratch_shapes=[pltpu.VMEM((216, LANES), f32)],
        compiler_params=LIMIT,
        name="views",
    )(rotation, shift, focal, means, scales, quats, grad_screen, visible)
    other = lax.ppermute(squares, "view", [(v, v ^ 1) for v in range(8)])
    squares = [jnp.maximum(squares, other)]
    for k in (1, 2, 3):
        pairs = [(v, (v + 2 * k) % 8) for v in range(8)]
        squares.append(lax.ppermute(squares[0], "view", pairs))

    start, index = pl.pallas_call(
        index_kernel,
        in_specs=[vmem()],
        out_specs=[vmem()] * 2,
        out_shape=[
            VMEM((8, LANES), i32),
            VMEM((BLOCKS, LANES), i32),
        ],
        compiler_params=LIMIT,
        name="index",
    )(mask)
    filled, total, branch, table = pl.pallas_call(
        fill_kernel,
        grid_spec=pltpu.PrefetchScalarGridSpec(
            num_scalar_prefetch=1,
            grid=(1,),
            in_specs=[
                smem(),
                smem(),
                whole(BLOCKS, LANES),
                whole(3, G_DEV),
                whole(3, G_DEV),
                whole(4, G_DEV),
                pl.BlockSpec((8, G_DEV), lambda i, w: (jnp.maximum(w[0] - 2, 0), 0)),
                pl.BlockSpec((8, G_DEV), lambda i, w: (jnp.maximum(w[0] - 1, 0), 0)),
            ],
            out_specs=[whole(BLOCKS, 8, LANES), smem(), smem(), smem()],
            scratch_shapes=[pltpu.VMEM((8, G_DEV), f32)],
        ),
        out_shape=[
            VMEM((BLOCKS, 8, LANES), f32),
            jax.ShapeDtypeStruct((1,), i32),
            jax.ShapeDtypeStruct((1,), i32),
            VMEM((3 * BLOCKS,), i32),
        ],
        compiler_params=LIMIT,
        name="fill",
    )(where, counts, start, index, means, scales, quats, attrs, attrs)
    outgoing = pl.pallas_call(
        add_kernel,
        in_specs=[smem()] + [vmem()] * 6,
        out_specs=vmem(),
        out_shape=VMEM((BLOCKS, 8, LANES), f32),
        input_output_aliases={6: 0},
        scratch_shapes=[pltpu.VMEM((2 * BLOCKS + 32, LANES), f32)],
        compiler_params=LIMIT,
        name="add",
    )(table, index, *squares, filled)

    def gather(cap):
        def go(where, table, outgoing, *squares):
            arrived = lax.all_to_all(
                outgoing.reshape(SHARDS, PER, 8, LANES), "gauss", 0, 0, tiled=True
            ).reshape(BLOCKS, 8, LANES)
            piece = pl.pallas_call(
                place_kernel,
                in_specs=[smem(), vmem()],
                out_specs=vmem(),
                out_shape=VMEM((4, cap, 8, LANES), f32),
                scratch_shapes=[pltpu.VMEM((cap + 1, 8, LANES), f32)],
                compiler_params=LIMIT,
                name="place",
            )(table, arrived)
            cores = [[0, 2, 4, 6], [1, 3, 5, 7]]
            own = lax.all_to_all(piece, "view", 0, 0, axis_index_groups=cores, tiled=True)
            other = lax.ppermute(own, "view", [(v, v ^ 1) for v in range(8)])
            peak = pl.pallas_call(
                peak_kernel,
                in_specs=[vmem()] * 4,
                out_specs=vmem(),
                out_shape=pltpu.MemorySpace.HBM((2, G_DEV), f32),
                scratch_shapes=[pltpu.VMEM((2 * BLOCKS + 32, LANES), f32)],
                compiler_params=LIMIT,
                name="peaks",
            )(*squares)
            begun = pl.pallas_call(
                own_kernel,
                in_specs=[smem(), vmem()],
                out_specs=pl.BlockSpec(memory_space=pl.ANY),
                out_shape=jax.ShapeDtypeStruct((ROWS, G_DEV), f32),
                scratch_shapes=[
                    pltpu.VMEM((8, 8, cap * LANES), f32),
                    pltpu.VMEM((8, max(BLOCKS - cap, 1) * LANES), f32),
                    pltpu.SemaphoreType.DMA((16,)),
                ],
                compiler_params=LIMIT,
                name="own",
            )(where, own)
            clones = pl.pallas_call(
                other_kernel,
                in_specs=[smem(), vmem(), pl.BlockSpec(memory_space=pl.ANY)],
                out_specs=pl.BlockSpec(memory_space=pl.ANY),
                out_shape=jax.ShapeDtypeStruct((ROWS, G_DEV), f32),
                input_output_aliases={2: 0},
                scratch_shapes=[
                    pltpu.VMEM((8, 8, cap * LANES), f32),
                    pltpu.SemaphoreType.DMA((8,)),
                ],
                compiler_params=LIMIT,
                name="other",
            )(where, other, begun)
            return peak, clones

        return go

    peak, clones = lax.switch(
        branch[0], [gather(cap) for cap in CAPS], where, table, outgoing, *squares
    )
    return (peak, clones, total[0])


def solution(mesh):
    return jax.shard_map(
        body,
        mesh=mesh,
        in_specs=(
            P(None, "gauss"),
            P(None, "gauss"),
            P(None, "gauss"),
            P(None, "gauss"),
            P("view", None, "gauss"),
            P("view", "gauss"),
            P("gauss"),
            P("view", None, None),
            P("view", None),
            P("view"),
        ),
        out_specs=(P(None, "gauss"), P(None, "gauss"), P()),
        check_vma=False,
    )
```

```python
import jax
import jax.numpy as jnp
from jax import lax
from jax.experimental import pallas as pl
from jax.experimental.pallas import tpu as pltpu
from jax.sharding import PartitionSpec as P

G_DEV = 16384
LANES = 128
BLOCKS = G_DEV // LANES
SHARDS = 32
PER = BLOCKS // SHARDS
VIEWS_DEV = 4
CAPS = (16, 32, 40, 48, 56, 64, 80, 96, BLOCKS)
ROWS = 61
LIMIT = pltpu.CompilerParams(vmem_limit_bytes=16 * 2**20)
SMEM = pltpu.MemorySpace.SMEM
VMEM = pltpu.MemorySpace.VMEM


def dot(a, b, dims=((1,), (0,))):
    return lax.dot_general(a, b, (dims, ((), ())), preferred_element_type=jnp.float32)


def where_1(cond):
    return jnp.where(cond, 1.0, 0.0).astype(jnp.bfloat16)


def count_kernel(mask_ref, count_ref):
    total = jnp.sum(jnp.sum(mask_ref[...], axis=0, keepdims=True), axis=1, keepdims=True)
    count_ref[...] = jnp.broadcast_to(total, (SHARDS, LANES))


def index_kernel(mask_ref, start_ref, index_ref):
    marked = mask_ref[...]
    ones = marked.astype(jnp.float32).astype(jnp.bfloat16)
    row = lax.broadcasted_iota(jnp.int32, (LANES, LANES), 0)
    lane = lax.broadcasted_iota(jnp.int32, (LANES, LANES), 1)
    full = jnp.ones((LANES, LANES), jnp.bfloat16)

    inclusive = dot(ones, where_1(row <= lane)).astype(jnp.int32)
    in_row = dot(ones, full)
    start = dot(where_1(row > lane), in_row.astype(jnp.bfloat16)).astype(jnp.int32)
    in_row_t = dot(jnp.ones((8, LANES), jnp.bfloat16), ones, ((1,), (1,)))
    start_ref[...] = dot(in_row_t.astype(jnp.bfloat16), where_1(row < lane)).astype(jnp.int32)

    moves = lane - inclusive + 1
    code = jnp.where(marked == 1, moves * 256 + lane, 0)
    for bit in range(7):
        moved = pltpu.roll(code, LANES - (1 << bit), 1)
        take = ((moved >> (8 + bit)) & 1) == 1
        leave = ((code >> (8 + bit)) & 1) == 1
        code = jnp.where(take, moved, jnp.where(leave, 0, code))
    first = start & (LANES - 1)
    nth = (lane - first) & (LANES - 1)
    source = jnp.take_along_axis(
        code & (LANES - 1), nth, axis=1, mode="promise_in_bounds"
    )
    valid = nth < in_row.astype(jnp.int32)
    here = jnp.where(valid, jnp.where(lane >= first, 256, 512), 0)
    index_ref[...] = source + here


def view_kernel(rot, trans, focal, means, scales, quats, grad, seen, out_ref, scr):
    width = 23

    def group(g, carry):
        for j in range(8):
            col = pl.ds(pl.multiple_of(g * 1024 + j * LANES, LANES), LANES)
            base = j * width
            scr[base : base + 3, :] = means[:, col]
            scr[base + 3 : base + 6, :] = scales[:, col]
            scr[base + 6 : base + 10, :] = quats[:, col]
            for v in range(VIEWS_DEV):
                scr[base + 10 + 2 * v : base + 12 + 2 * v, :] = grad[v, :, col]
            scr[base + 18 : base + 22, :] = seen[:, col].astype(jnp.float32)

        def comp(r):
            return scr[pl.ds(r, 8, stride=width), :]

        m = [comp(i) for i in range(3)]
        sc = [comp(3 + i) for i in range(3)]
        q = [comp(6 + i) for i in range(4)]
        norm = q[0] * q[0] + q[1] * q[1] + q[2] * q[2] + q[3] * q[3]
        inv = 1.0 / jnp.sqrt(norm + 0.25)
        w, x, y, z = (c * inv for c in q)
        rq = [
            [1 - 2 * (y * y + z * z), 2 * (x * y - w * z), 2 * (x * z + w * y)],
            [2 * (x * y + w * z), 1 - 2 * (x * x + z * z), 2 * (y * z - w * x)],
            [2 * (x * z - w * y), 2 * (y * z + w * x), 1 - 2 * (x * x + y * y)],
        ]
        factor = [[rq[i][j] * sc[j] for j in range(3)] for i in range(3)]
        gmax = jnp.zeros((8, LANES), jnp.float32)
        lmax = jnp.zeros((8, LANES), jnp.float32)
        for v in range(VIEWS_DEV):
            r = [[rot[i, v, j] for j in range(3)] for i in range(3)]
            f = focal[0, v]
            p = [r[i][0] * m[0] + r[i][1] * m[1] + r[i][2] * m[2] + trans[v, i] for i in range(3)]
            over = 1.0 / jnp.maximum(p[2], 1.0)
            j00 = f * over
            j02 = -(j00 * p[0]) * over
            j12 = -(j00 * p[1]) * over
            first = [j00 * r[0][j] + j02 * r[2][j] for j in range(3)]
            second = [j00 * r[1][j] + j12 * r[2][j] for j in range(3)]
            pr = [sum(first[j] * factor[j][k] for j in range(3)) for k in range(3)]
            qr = [sum(second[j] * factor[j][k] for j in range(3)) for k in range(3)]
            a = pr[0] * pr[0] + pr[1] * pr[1] + pr[2] * pr[2] + 0.3
            c = qr[0] * qr[0] + qr[1] * qr[1] + qr[2] * qr[2] + 0.3
            b = pr[0] * qr[0] + pr[1] * qr[1] + pr[2] * qr[2]
            half = 0.5 * (a - c)
            lam = 0.5 * (a + c) + jnp.sqrt(half * half + b * b + 0.01)
            vis = comp(18 + v)
            g0 = comp(10 + 2 * v)
            g1 = comp(11 + 2 * v)
            gmax = jnp.maximum(gmax, (g0 * g0 + g1 * g1) * vis)
            lmax = jnp.maximum(lmax, lam * vis)
        rows = pl.ds(pl.multiple_of(g * 8, 8), 8)
        out_ref[0, rows, :] = gmax
        out_ref[1, rows, :] = lmax
        return carry

    lax.fori_loop(0, means.shape[1] // 1024, group, 0)


def fill_kernel(
    where, counts, start, index, means, scales, quats, low, high,
    out_ref, sums_ref, pick_ref, table, rows
):
    view = where[0]

    @pl.when(view == 0)
    def _():
        rows[0:3, :] = means[...]
        rows[3:6, :] = scales[...]
        rows[6:8, :] = quats[0:2, :]

    @pl.when(view == 1)
    def _():
        rows[0:2, :] = quats[2:4, :]

    @pl.when(view > 1)
    def _():
        rows[0:2, :] = low[6:8, :]

    @pl.when((view > 0) & (view < 7))
    def _():
        rows[2:8, :] = high[0:6, :]

    @pl.when(view == 7)
    def _():
        rows[2:3, :] = high[0:1, :]
        rows[3:8, :] = jnp.zeros((5, G_DEV), jnp.float32)

    zero = jnp.zeros((8, LANES), jnp.float32)
    for i in range(BLOCKS):
        out_ref[i] = zero

    mine = where[1]
    total = offset = used = jnp.int32(0)
    for s in range(SHARDS):
        offset = jnp.where(s == mine, used, offset)
        local = (mine - used) & (SHARDS - 1)
        first = (used + local) >> 5
        for w in range(PER):
            table[BLOCKS + s * PER + w] = first + w
        count = counts[s, 0]
        total = total + count
        used = used + ((count + LANES - 1) >> 7)
    sums_ref[0] = total
    pick = jnp.int32(0)
    for cap in CAPS[:-1]:
        pick = pick + jnp.where(used > cap * SHARDS, 1, 0)
    pick_ref[0] = pick
    table[2 * BLOCKS] = view

    def place_of(block):
        return ((offset + block) & (SHARDS - 1)) * PER + (block >> 5)

    def some(i, carry):
        for j in range(32):
            b = i * 32 + j
            block = start[0, b] >> 7
            here = place_of(block)
            after = place_of(jnp.minimum(block + 1, BLOCKS - 1))
            table[b] = here + (after << 8)
            code = jnp.broadcast_to(index[pl.ds(b, 1), :], (8, LANES))
            tile = rows[:, pl.ds(pl.multiple_of(b * LANES, LANES), LANES)]
            packed = jnp.take_along_axis(
                tile, code & (LANES - 1), axis=1, mode="promise_in_bounds"
            )
            pltpu.store(out_ref.at[here], packed, mask=(code & 256) != 0)
            pltpu.store(out_ref.at[after], packed, mask=(code & 512) != 0)
        return carry

    lax.fori_loop(0, BLOCKS // 32, some, 0)


def top_of(squares, k, at):
    a, b, c, d = (sq[k, at, :] for sq in squares)
    return jnp.maximum(jnp.maximum(a, b), jnp.maximum(c, d))


def add_kernel(table, index, sq0, sq1, sq2, sq3, filled, out_ref, pairs):
    @pl.when(table[2 * BLOCKS] == 7)
    def _():
        for g in range(BLOCKS // 8):
            at = slice(8 * g, 8 * g + 8)
            lanes = index[at, :] & (LANES - 1)
            for k in range(2):
                root = jnp.sqrt(top_of((sq0, sq1, sq2, sq3), k, at))
                pairs[pl.ds(16 * g + k, 8, stride=2), :] = jnp.take_along_axis(
                    root if k == 0 else 3.0 * root, lanes, axis=1, mode="promise_in_bounds"
                )
        for b in range(BLOCKS):
            both = table[b]
            code = jnp.broadcast_to(index[b : b + 1, :], (2, LANES))
            two = pairs[2 * b : 2 * b + 2, :]
            pltpu.store(out_ref.at[both & 255, 3:5, :], two, mask=(code & 256) != 0)
            pltpu.store(out_ref.at[both >> 8, 3:5, :], two, mask=(code & 512) != 0)


def place_kernel(table, arrived, out_ref, slots):
    cap = out_ref.shape[1]
    zero = jnp.zeros((8, LANES), jnp.float32)
    for i in range(cap):
        slots[i] = zero
    for i in range(BLOCKS):
        slots[jnp.minimum(table[BLOCKS + i], cap)] = arrived[i]
    for i in range(cap):
        tile = slots[i]
        for x in range(4):
            out_ref[x, i] = tile


def row_copy(buf, out_ref, sems, r, columns):
    rows = min(8, ROWS - 8 * r)
    return pltpu.make_async_copy(
        buf.at[r, 0:rows, columns], out_ref.at[8 * r : 8 * r + rows, columns], sems.at[r]
    )


def own_kernel(
    where, own, sq0, sq1, sq2, sq3, out_ref, peak_ref, buf, zeros, pairs, peaks, sems
):
    cap = own.shape[1]
    core = where[0] & 1

    def clear(r):
        rows = min(8, ROWS - 8 * r)
        return pltpu.make_async_copy(
            zeros.at[0:rows, :],
            out_ref.at[8 * r : 8 * r + rows, cap * LANES : G_DEV],
            sems.at[8 + r],
        )

    if cap < BLOCKS:
        for i in range(BLOCKS - cap):
            zeros[:, i * LANES : (i + 1) * LANES] = jnp.zeros((8, LANES), jnp.float32)
        for r in range(8):
            clear(r).start()
    for half in range(2):

        @pl.when(core == half)
        def _():
            for r in range(half, 8, 2):
                for i in range(cap):
                    buf[r, :, i * LANES : (i + 1) * LANES] = own[r // 2, i]
                row_copy(buf, out_ref, sems, r, slice(0, cap * LANES)).start()

    for g in range(BLOCKS // 8):
        at = slice(8 * g, 8 * g + 8)
        norm = jnp.sqrt(top_of((sq0, sq1, sq2, sq3), 0, at))
        radius = 3.0 * jnp.sqrt(top_of((sq0, sq1, sq2, sq3), 1, at))
        pairs[pl.ds(16 * g, 8, stride=2), :] = norm
        pairs[pl.ds(16 * g + 1, 8, stride=2), :] = radius
    for b in range(BLOCKS):
        peaks[:, b * LANES : (b + 1) * LANES] = pairs[2 * b : 2 * b + 2, :]
    peak_copy = pltpu.make_async_copy(peaks, peak_ref, sems.at[16])
    peak_copy.start()

    for half in range(2):

        @pl.when(core == half)
        def _():
            for r in range(half, 8, 2):
                row_copy(buf, out_ref, sems, r, slice(0, cap * LANES)).wait()

    if cap < BLOCKS:
        for r in range(8):
            clear(r).wait()
    peak_copy.wait()


def other_kernel(where, other, begun, out_ref, buf, sems):
    cap = other.shape[1]
    core = where[0] & 1
    for half in range(2):

        @pl.when(core == half)
        def _():
            for r in range(1 - half, 8, 2):
                for i in range(cap):
                    buf[r, :, i * LANES : (i + 1) * LANES] = other[r // 2, i]
                row_copy(buf, out_ref, sems, r, slice(0, cap * LANES)).start()
            for r in range(1 - half, 8, 2):
                row_copy(buf, out_ref, sems, r, slice(0, cap * LANES)).wait()


def smem():
    return pl.BlockSpec(memory_space=SMEM)


def vmem():
    return pl.BlockSpec(memory_space=VMEM)


def body(means, scales, quats, attrs, grad_screen, visible, clone_mask, rotation, shift, focal):
    f32, i32 = jnp.float32, jnp.int32
    view = lax.axis_index("view")
    where = jnp.stack([view, lax.axis_index("gauss")]).astype(i32)

    def whole(*shape):
        return pl.BlockSpec(shape, lambda i, w: (0,) * len(shape))

    mask = clone_mask.reshape(BLOCKS, LANES)
    rotation, focal = rotation.transpose(1, 0, 2), focal.reshape(1, VIEWS_DEV)
    mask, means, scales, quats, attrs, grad_screen, visible, rotation, shift, focal = (
        pltpu.with_memory_space_constraint(x, pltpu.MemorySpace.HBM)
        for x in (
            mask, means, scales, quats, attrs, grad_screen, visible, rotation, shift, focal
        )
    )
    count = pl.pallas_call(
        count_kernel,
        in_specs=[vmem()],
        out_specs=vmem(),
        out_shape=VMEM((SHARDS, LANES), i32),
        compiler_params=LIMIT,
        name="count",
    )(mask)
    counts = lax.all_to_all(count, "gauss", 0, 0, tiled=True)

    squares = pl.pallas_call(
        view_kernel,
        in_specs=[smem()] * 3 + [vmem()] * 5,
        out_specs=vmem(),
        out_shape=VMEM((2, BLOCKS, LANES), f32),
        scratch_shapes=[pltpu.VMEM((216, LANES), f32)],
        compiler_params=LIMIT,
        name="views",
    )(rotation, shift, focal, means, scales, quats, grad_screen, visible)
    other = lax.ppermute(squares, "view", [(v, v ^ 1) for v in range(8)])
    squares = [jnp.maximum(squares, other)]
    for k in (1, 2, 3):
        pairs = [(v, (v + 2 * k) % 8) for v in range(8)]
        squares.append(lax.ppermute(squares[0], "view", pairs))

    start, index = pl.pallas_call(
        index_kernel,
        in_specs=[vmem()],
        out_specs=[vmem()] * 2,
        out_shape=[
            VMEM((8, LANES), i32),
            VMEM((BLOCKS, LANES), i32),
        ],
        compiler_params=LIMIT,
        name="index",
    )(mask)
    filled, total, branch, table = pl.pallas_call(
        fill_kernel,
        grid_spec=pltpu.PrefetchScalarGridSpec(
            num_scalar_prefetch=1,
            grid=(1,),
            in_specs=[
                smem(),
                smem(),
                whole(BLOCKS, LANES),
                whole(3, G_DEV),
                whole(3, G_DEV),
                whole(4, G_DEV),
                pl.BlockSpec((8, G_DEV), lambda i, w: (jnp.maximum(w[0] - 2, 0), 0)),
                pl.BlockSpec((8, G_DEV), lambda i, w: (jnp.maximum(w[0] - 1, 0), 0)),
            ],
            out_specs=[whole(BLOCKS, 8, LANES), smem(), smem(), smem()],
            scratch_shapes=[pltpu.VMEM((8, G_DEV), f32)],
        ),
        out_shape=[
            VMEM((BLOCKS, 8, LANES), f32),
            jax.ShapeDtypeStruct((1,), i32),
            jax.ShapeDtypeStruct((1,), i32),
            VMEM((3 * BLOCKS,), i32),
        ],
        compiler_params=LIMIT,
        name="fill",
    )(where, counts, start, index, means, scales, quats, attrs, attrs)
    outgoing = pl.pallas_call(
        add_kernel,
        in_specs=[smem()] + [vmem()] * 6,
        out_specs=vmem(),
        out_shape=VMEM((BLOCKS, 8, LANES), f32),
        input_output_aliases={6: 0},
        scratch_shapes=[pltpu.VMEM((2 * BLOCKS + 32, LANES), f32)],
        compiler_params=LIMIT,
        name="add",
    )(table, index, *squares, filled)

    def gather(cap):
        def go(where, table, outgoing, *squares):
            arrived = lax.all_to_all(
                outgoing.reshape(SHARDS, PER, 8, LANES), "gauss", 0, 0, tiled=True
            ).reshape(BLOCKS, 8, LANES)
            piece = pl.pallas_call(
                place_kernel,
                in_specs=[smem(), vmem()],
                out_specs=vmem(),
                out_shape=VMEM((4, cap, 8, LANES), f32),
                scratch_shapes=[pltpu.VMEM((cap + 1, 8, LANES), f32)],
                compiler_params=LIMIT,
                name="place",
            )(table, arrived)
            cores = [[0, 2, 4, 6], [1, 3, 5, 7]]
            own = lax.all_to_all(piece, "view", 0, 0, axis_index_groups=cores, tiled=True)
            other = lax.ppermute(own, "view", [(v, v ^ 1) for v in range(8)])
            begun, peak = pl.pallas_call(
                own_kernel,
                in_specs=[smem()] + [vmem()] * 5,
                out_specs=[pl.BlockSpec(memory_space=pl.ANY)] * 2,
                out_shape=[
                    jax.ShapeDtypeStruct((ROWS, G_DEV), f32),
                    pltpu.MemorySpace.HBM((2, G_DEV), f32),
                ],
                scratch_shapes=[
                    pltpu.VMEM((8, 8, cap * LANES), f32),
                    pltpu.VMEM((8, max(BLOCKS - cap, 1) * LANES), f32),
                    pltpu.VMEM((2 * BLOCKS + 32, LANES), f32),
                    pltpu.VMEM((2, G_DEV), f32),
                    pltpu.SemaphoreType.DMA((17,)),
                ],
                compiler_params=LIMIT,
                name="own",
            )(where, own, *squares)
            clones = pl.pallas_call(
                other_kernel,
                in_specs=[smem(), vmem(), pl.BlockSpec(memory_space=pl.ANY)],
                out_specs=pl.BlockSpec(memory_space=pl.ANY),
                out_shape=jax.ShapeDtypeStruct((ROWS, G_DEV), f32),
                input_output_aliases={2: 0},
                scratch_shapes=[
                    pltpu.VMEM((8, 8, cap * LANES), f32),
                    pltpu.SemaphoreType.DMA((8,)),
                ],
                compiler_params=LIMIT,
                name="other",
            )(where, other, begun)
            return peak, clones

        return go

    peak, clones = lax.switch(
        branch[0], [gather(cap) for cap in CAPS], where, table, outgoing, *squares
    )
    return (peak, clones, total[0])


def solution(mesh):
    return jax.shard_map(
        body,
        mesh=mesh,
        in_specs=(
            P(None, "gauss"),
            P(None, "gauss"),
            P(None, "gauss"),
            P(None, "gauss"),
            P("view", None, "gauss"),
            P("view", "gauss"),
            P("gauss"),
            P("view", None, None),
            P("view", None),
            P("view"),
        ),
        out_specs=(P(None, "gauss"), P(None, "gauss"), P()),
        check_vma=False,
    )
```

```python
import jax
import jax.numpy as jnp
from jax import lax
from jax.experimental import pallas as pl
from jax.experimental.pallas import tpu as pltpu
from jax.sharding import PartitionSpec as P

G_DEV = 16384
LANES = 128
BLOCKS = G_DEV // LANES
SHARDS = 32
PER = BLOCKS // SHARDS
VIEWS_DEV = 4
CAPS = (16, 32, 40, 48, 56, 64, 80, 96, BLOCKS)
ROWS = 61
LIMIT = pltpu.CompilerParams(vmem_limit_bytes=16 * 2**20)
SMEM = pltpu.MemorySpace.SMEM
VMEM = pltpu.MemorySpace.VMEM


def dot(a, b, dims=((1,), (0,))):
    return lax.dot_general(a, b, (dims, ((), ())), preferred_element_type=jnp.float32)


def where_1(cond):
    return jnp.where(cond, 1.0, 0.0).astype(jnp.bfloat16)


def count_kernel(mask_ref, count_ref):
    total = jnp.sum(jnp.sum(mask_ref[...], axis=0, keepdims=True), axis=1, keepdims=True)
    count_ref[...] = jnp.broadcast_to(total, (SHARDS, LANES))


def index_kernel(mask_ref, start_ref, index_ref):
    marked = mask_ref[...]
    ones = marked.astype(jnp.float32).astype(jnp.bfloat16)
    row = lax.broadcasted_iota(jnp.int32, (LANES, LANES), 0)
    lane = lax.broadcasted_iota(jnp.int32, (LANES, LANES), 1)
    full = jnp.ones((LANES, LANES), jnp.bfloat16)

    inclusive = dot(ones, where_1(row <= lane)).astype(jnp.int32)
    in_row = dot(ones, full)
    start = dot(where_1(row > lane), in_row.astype(jnp.bfloat16)).astype(jnp.int32)
    in_row_t = dot(jnp.ones((8, LANES), jnp.bfloat16), ones, ((1,), (1,)))
    start_ref[...] = dot(in_row_t.astype(jnp.bfloat16), where_1(row < lane)).astype(jnp.int32)

    moves = lane - inclusive + 1
    code = jnp.where(marked == 1, moves * 256 + lane, 0)
    for bit in range(7):
        moved = pltpu.roll(code, LANES - (1 << bit), 1)
        take = ((moved >> (8 + bit)) & 1) == 1
        leave = ((code >> (8 + bit)) & 1) == 1
        code = jnp.where(take, moved, jnp.where(leave, 0, code))
    first = start & (LANES - 1)
    nth = (lane - first) & (LANES - 1)
    source = jnp.take_along_axis(
        code & (LANES - 1), nth, axis=1, mode="promise_in_bounds"
    )
    valid = nth < in_row.astype(jnp.int32)
    here = jnp.where(valid, jnp.where(lane >= first, 256, 512), 0)
    index_ref[...] = source + here


def view_kernel(rot, trans, focal, means, scales, quats, grad, seen, out_ref, scr):
    width = 23

    def group(g, carry):
        for j in range(8):
            col = pl.ds(pl.multiple_of(g * 1024 + j * LANES, LANES), LANES)
            base = j * width
            scr[base : base + 3, :] = means[:, col]
            scr[base + 3 : base + 6, :] = scales[:, col]
            scr[base + 6 : base + 10, :] = quats[:, col]
            for v in range(VIEWS_DEV):
                scr[base + 10 + 2 * v : base + 12 + 2 * v, :] = grad[v, :, col]
            scr[base + 18 : base + 22, :] = seen[:, col].astype(jnp.float32)

        def comp(r):
            return scr[pl.ds(r, 8, stride=width), :]

        m = [comp(i) for i in range(3)]
        sc = [comp(3 + i) for i in range(3)]
        q = [comp(6 + i) for i in range(4)]
        norm = q[0] * q[0] + q[1] * q[1] + q[2] * q[2] + q[3] * q[3]
        inv = 1.0 / jnp.sqrt(norm + 0.25)
        w, x, y, z = (c * inv for c in q)
        rq = [
            [1 - 2 * (y * y + z * z), 2 * (x * y - w * z), 2 * (x * z + w * y)],
            [2 * (x * y + w * z), 1 - 2 * (x * x + z * z), 2 * (y * z - w * x)],
            [2 * (x * z - w * y), 2 * (y * z + w * x), 1 - 2 * (x * x + y * y)],
        ]
        factor = [[rq[i][j] * sc[j] for j in range(3)] for i in range(3)]
        gmax = jnp.zeros((8, LANES), jnp.float32)
        lmax = jnp.zeros((8, LANES), jnp.float32)
        for v in range(VIEWS_DEV):
            r = [[rot[i, v, j] for j in range(3)] for i in range(3)]
            f = focal[0, v]
            p = [r[i][0] * m[0] + r[i][1] * m[1] + r[i][2] * m[2] + trans[v, i] for i in range(3)]
            over = 1.0 / jnp.maximum(p[2], 1.0)
            j00 = f * over
            j02 = -(j00 * p[0]) * over
            j12 = -(j00 * p[1]) * over
            first = [j00 * r[0][j] + j02 * r[2][j] for j in range(3)]
            second = [j00 * r[1][j] + j12 * r[2][j] for j in range(3)]
            pr = [sum(first[j] * factor[j][k] for j in range(3)) for k in range(3)]
            qr = [sum(second[j] * factor[j][k] for j in range(3)) for k in range(3)]
            a = pr[0] * pr[0] + pr[1] * pr[1] + pr[2] * pr[2] + 0.3
            c = qr[0] * qr[0] + qr[1] * qr[1] + qr[2] * qr[2] + 0.3
            b = pr[0] * qr[0] + pr[1] * qr[1] + pr[2] * qr[2]
            half = 0.5 * (a - c)
            lam = 0.5 * (a + c) + jnp.sqrt(half * half + b * b + 0.01)
            vis = comp(18 + v)
            g0 = comp(10 + 2 * v)
            g1 = comp(11 + 2 * v)
            gmax = jnp.maximum(gmax, (g0 * g0 + g1 * g1) * vis)
            lmax = jnp.maximum(lmax, lam * vis)
        rows = pl.ds(pl.multiple_of(g * 8, 8), 8)
        out_ref[0, rows, :] = gmax
        out_ref[1, rows, :] = lmax
        return carry

    lax.fori_loop(0, means.shape[1] // 1024, group, 0)


def fill_kernel(
    where, counts, start, index, means, scales, quats, low, high,
    out_ref, pick_ref, table, rows
):
    view = where[0]

    @pl.when(view == 0)
    def _():
        rows[0:3, :] = means[...]
        rows[3:6, :] = scales[...]
        rows[6:8, :] = quats[0:2, :]

    @pl.when(view == 1)
    def _():
        rows[0:2, :] = quats[2:4, :]

    @pl.when(view > 1)
    def _():
        rows[0:2, :] = low[6:8, :]

    @pl.when((view > 0) & (view < 7))
    def _():
        rows[2:8, :] = high[0:6, :]

    @pl.when(view == 7)
    def _():
        rows[2:3, :] = high[0:1, :]
        rows[3:8, :] = jnp.zeros((5, G_DEV), jnp.float32)

    zero = jnp.zeros((8, LANES), jnp.float32)
    for i in range(BLOCKS):
        out_ref[i] = zero

    mine = where[1]
    total = offset = used = jnp.int32(0)
    for s in range(SHARDS):
        offset = jnp.where(s == mine, used, offset)
        local = (mine - used) & (SHARDS - 1)
        first = (used + local) >> 5
        for w in range(PER):
            table[BLOCKS + s * PER + w] = first + w
        count = counts[s, 0]
        total = total + count
        used = used + ((count + LANES - 1) >> 7)
    table[2 * BLOCKS + 1] = total
    pick = jnp.int32(0)
    for cap in CAPS[:-1]:
        pick = pick + jnp.where(used > cap * SHARDS, 1, 0)
    pick_ref[0] = pick
    table[2 * BLOCKS] = view

    def place_of(block):
        return ((offset + block) & (SHARDS - 1)) * PER + (block >> 5)

    def some(i, carry):
        for j in range(32):
            b = i * 32 + j
            block = start[0, b] >> 7
            here = place_of(block)
            after = place_of(jnp.minimum(block + 1, BLOCKS - 1))
            table[b] = here + (after << 8)
            code = jnp.broadcast_to(index[pl.ds(b, 1), :], (8, LANES))
            tile = rows[:, pl.ds(pl.multiple_of(b * LANES, LANES), LANES)]
            packed = jnp.take_along_axis(
                tile, code & (LANES - 1), axis=1, mode="promise_in_bounds"
            )
            pltpu.store(out_ref.at[here], packed, mask=(code & 256) != 0)
            pltpu.store(out_ref.at[after], packed, mask=(code & 512) != 0)
        return carry

    lax.fori_loop(0, BLOCKS // 32, some, 0)


def top_of(squares, k, at):
    a, b, c, d = (sq[k, at, :] for sq in squares)
    return jnp.maximum(jnp.maximum(a, b), jnp.maximum(c, d))


def add_kernel(table, index, sq0, sq1, sq2, sq3, filled, out_ref, pairs):
    @pl.when(table[2 * BLOCKS] == 7)
    def _():
        for g in range(BLOCKS // 8):
            at = slice(8 * g, 8 * g + 8)
            lanes = index[at, :] & (LANES - 1)
            for k in range(2):
                root = jnp.sqrt(top_of((sq0, sq1, sq2, sq3), k, at))
                pairs[pl.ds(16 * g + k, 8, stride=2), :] = jnp.take_along_axis(
                    root if k == 0 else 3.0 * root, lanes, axis=1, mode="promise_in_bounds"
                )
        for b in range(BLOCKS):
            both = table[b]
            code = jnp.broadcast_to(index[b : b + 1, :], (2, LANES))
            two = pairs[2 * b : 2 * b + 2, :]
            pltpu.store(out_ref.at[both & 255, 3:5, :], two, mask=(code & 256) != 0)
            pltpu.store(out_ref.at[both >> 8, 3:5, :], two, mask=(code & 512) != 0)


def place_kernel(table, arrived, out_ref, slots):
    cap = out_ref.shape[1]
    zero = jnp.zeros((8, LANES), jnp.float32)
    for i in range(cap):
        slots[i] = zero
    for i in range(BLOCKS):
        slots[jnp.minimum(table[BLOCKS + i], cap)] = arrived[i]
    for i in range(cap):
        tile = slots[i]
        for x in range(4):
            out_ref[x, i] = tile


def row_copy(buf, out_ref, sems, r, columns):
    rows = min(8, ROWS - 8 * r)
    return pltpu.make_async_copy(
        buf.at[r, 0:rows, columns], out_ref.at[8 * r : 8 * r + rows, columns], sems.at[r]
    )


def own_kernel(
    table, own, sq0, sq1, sq2, sq3,
    out_ref, peak_ref, total_ref, buf, zeros, pairs, peaks, sems
):
    cap = own.shape[1]
    core = table[2 * BLOCKS] & 1
    total_ref[0] = table[2 * BLOCKS + 1]

    def clear(r):
        rows = min(8, ROWS - 8 * r)
        return pltpu.make_async_copy(
            zeros.at[0:rows, :],
            out_ref.at[8 * r : 8 * r + rows, cap * LANES : G_DEV],
            sems.at[8 + r],
        )

    if cap < BLOCKS:
        for i in range(BLOCKS - cap):
            zeros[:, i * LANES : (i + 1) * LANES] = jnp.zeros((8, LANES), jnp.float32)
        for r in range(8):
            clear(r).start()
    for half in range(2):

        @pl.when(core == half)
        def _():
            for r in range(half, 8, 2):
                for i in range(cap):
                    buf[r, :, i * LANES : (i + 1) * LANES] = own[r // 2, i]
                row_copy(buf, out_ref, sems, r, slice(0, cap * LANES)).start()

    for g in range(BLOCKS // 8):
        at = slice(8 * g, 8 * g + 8)
        norm = jnp.sqrt(top_of((sq0, sq1, sq2, sq3), 0, at))
        radius = 3.0 * jnp.sqrt(top_of((sq0, sq1, sq2, sq3), 1, at))
        pairs[pl.ds(16 * g, 8, stride=2), :] = norm
        pairs[pl.ds(16 * g + 1, 8, stride=2), :] = radius
    for b in range(BLOCKS):
        peaks[:, b * LANES : (b + 1) * LANES] = pairs[2 * b : 2 * b + 2, :]
    peak_copy = pltpu.make_async_copy(peaks, peak_ref, sems.at[16])
    peak_copy.start()

    for half in range(2):

        @pl.when(core == half)
        def _():
            for r in range(half, 8, 2):
                row_copy(buf, out_ref, sems, r, slice(0, cap * LANES)).wait()

    if cap < BLOCKS:
        for r in range(8):
            clear(r).wait()
    peak_copy.wait()


def other_kernel(table, other, begun, out_ref, buf, sems):
    cap = other.shape[1]
    core = table[2 * BLOCKS] & 1
    for half in range(2):

        @pl.when(core == half)
        def _():
            for r in range(1 - half, 8, 2):
                for i in range(cap):
                    buf[r, :, i * LANES : (i + 1) * LANES] = other[r // 2, i]
                row_copy(buf, out_ref, sems, r, slice(0, cap * LANES)).start()
            for r in range(1 - half, 8, 2):
                row_copy(buf, out_ref, sems, r, slice(0, cap * LANES)).wait()


def smem():
    return pl.BlockSpec(memory_space=SMEM)


def vmem():
    return pl.BlockSpec(memory_space=VMEM)


def body(means, scales, quats, attrs, grad_screen, visible, clone_mask, rotation, shift, focal):
    f32, i32 = jnp.float32, jnp.int32
    view = lax.axis_index("view")
    where = jnp.stack([view, lax.axis_index("gauss")]).astype(i32)

    def whole(*shape):
        return pl.BlockSpec(shape, lambda i, w: (0,) * len(shape))

    mask = clone_mask.reshape(BLOCKS, LANES)
    rotation, focal = rotation.transpose(1, 0, 2), focal.reshape(1, VIEWS_DEV)
    mask, means, scales, quats, attrs, grad_screen, visible, rotation, shift, focal = (
        pltpu.with_memory_space_constraint(x, pltpu.MemorySpace.HBM)
        for x in (
            mask, means, scales, quats, attrs, grad_screen, visible, rotation, shift, focal
        )
    )
    count = pl.pallas_call(
        count_kernel,
        in_specs=[vmem()],
        out_specs=vmem(),
        out_shape=VMEM((SHARDS, LANES), i32),
        compiler_params=LIMIT,
        name="count",
    )(mask)
    counts = lax.all_to_all(count, "gauss", 0, 0, tiled=True)

    squares = pl.pallas_call(
        view_kernel,
        in_specs=[smem()] * 3 + [vmem()] * 5,
        out_specs=vmem(),
        out_shape=VMEM((2, BLOCKS, LANES), f32),
        scratch_shapes=[pltpu.VMEM((216, LANES), f32)],
        compiler_params=LIMIT,
        name="views",
    )(rotation, shift, focal, means, scales, quats, grad_screen, visible)
    other = lax.ppermute(squares, "view", [(v, v ^ 1) for v in range(8)])
    squares = [jnp.maximum(squares, other)]
    for k in (1, 2, 3):
        pairs = [(v, (v + 2 * k) % 8) for v in range(8)]
        squares.append(lax.ppermute(squares[0], "view", pairs))

    start, index = pl.pallas_call(
        index_kernel,
        in_specs=[vmem()],
        out_specs=[vmem()] * 2,
        out_shape=[
            VMEM((8, LANES), i32),
            VMEM((BLOCKS, LANES), i32),
        ],
        compiler_params=LIMIT,
        name="index",
    )(mask)
    filled, branch, table = pl.pallas_call(
        fill_kernel,
        grid_spec=pltpu.PrefetchScalarGridSpec(
            num_scalar_prefetch=1,
            grid=(1,),
            in_specs=[
                smem(),
                smem(),
                whole(BLOCKS, LANES),
                whole(3, G_DEV),
                whole(3, G_DEV),
                whole(4, G_DEV),
                pl.BlockSpec((8, G_DEV), lambda i, w: (jnp.maximum(w[0] - 2, 0), 0)),
                pl.BlockSpec((8, G_DEV), lambda i, w: (jnp.maximum(w[0] - 1, 0), 0)),
            ],
            out_specs=[whole(BLOCKS, 8, LANES), smem(), smem()],
            scratch_shapes=[pltpu.VMEM((8, G_DEV), f32)],
        ),
        out_shape=[
            VMEM((BLOCKS, 8, LANES), f32),
            SMEM((1,), i32),
            SMEM((3 * BLOCKS,), i32),
        ],
        compiler_params=LIMIT,
        name="fill",
    )(where, counts, start, index, means, scales, quats, attrs, attrs)
    outgoing = pl.pallas_call(
        add_kernel,
        in_specs=[smem()] + [vmem()] * 6,
        out_specs=vmem(),
        out_shape=VMEM((BLOCKS, 8, LANES), f32),
        input_output_aliases={6: 0},
        scratch_shapes=[pltpu.VMEM((2 * BLOCKS + 32, LANES), f32)],
        compiler_params=LIMIT,
        name="add",
    )(table, index, *squares, filled)

    def gather(cap):
        def go(table, outgoing, *squares):
            arrived = lax.all_to_all(
                outgoing.reshape(SHARDS, PER, 8, LANES), "gauss", 0, 0, tiled=True
            ).reshape(BLOCKS, 8, LANES)
            piece = pl.pallas_call(
                place_kernel,
                in_specs=[smem(), vmem()],
                out_specs=vmem(),
                out_shape=VMEM((4, cap, 8, LANES), f32),
                scratch_shapes=[pltpu.VMEM((cap + 1, 8, LANES), f32)],
                compiler_params=LIMIT,
                name="place",
            )(table, arrived)
            cores = [[0, 2, 4, 6], [1, 3, 5, 7]]
            own = lax.all_to_all(piece, "view", 0, 0, axis_index_groups=cores, tiled=True)
            other = lax.ppermute(own, "view", [(v, v ^ 1) for v in range(8)])
            begun, peak, total = pl.pallas_call(
                own_kernel,
                in_specs=[smem()] + [vmem()] * 5,
                out_specs=[pl.BlockSpec(memory_space=pl.ANY)] * 2 + [smem()],
                out_shape=[
                    jax.ShapeDtypeStruct((ROWS, G_DEV), f32),
                    pltpu.MemorySpace.HBM((2, G_DEV), f32),
                    pltpu.MemorySpace.HBM((1,), i32),
                ],
                scratch_shapes=[
                    pltpu.VMEM((8, 8, cap * LANES), f32),
                    pltpu.VMEM((8, max(BLOCKS - cap, 1) * LANES), f32),
                    pltpu.VMEM((2 * BLOCKS + 32, LANES), f32),
                    pltpu.VMEM((2, G_DEV), f32),
                    pltpu.SemaphoreType.DMA((17,)),
                ],
                compiler_params=LIMIT,
                name="own",
            )(table, own, *squares)
            clones = pl.pallas_call(
                other_kernel,
                in_specs=[smem(), vmem(), pl.BlockSpec(memory_space=pl.ANY)],
                out_specs=pl.BlockSpec(memory_space=pl.ANY),
                out_shape=jax.ShapeDtypeStruct((ROWS, G_DEV), f32),
                input_output_aliases={2: 0},
                scratch_shapes=[
                    pltpu.VMEM((8, 8, cap * LANES), f32),
                    pltpu.SemaphoreType.DMA((8,)),
                ],
                compiler_params=LIMIT,
                name="other",
            )(table, other, begun)
            return peak, clones, total

        return go

    peak, clones, total = lax.switch(
        branch[0], [gather(cap) for cap in CAPS], table, outgoing, *squares
    )
    return (peak, clones, total[0])


def solution(mesh):
    return jax.shard_map(
        body,
        mesh=mesh,
        in_specs=(
            P(None, "gauss"),
            P(None, "gauss"),
            P(None, "gauss"),
            P(None, "gauss"),
            P("view", None, "gauss"),
            P("view", "gauss"),
            P("gauss"),
            P("view", None, None),
            P("view", None),
            P("view"),
        ),
        out_specs=(P(None, "gauss"), P(None, "gauss"), P()),
        check_vma=False,
    )
```

```python
import jax
import jax.numpy as jnp
from jax import lax
from jax.experimental import pallas as pl
from jax.experimental.pallas import tpu as pltpu
from jax.sharding import PartitionSpec as P

G_DEV = 16384
LANES = 128
BLOCKS = G_DEV // LANES
SHARDS = 32
PER = BLOCKS // SHARDS
VIEWS_DEV = 4
CAPS = (16, 32, 40, 48, 56, 64, 80, 96, BLOCKS)
ROWS = 61
LIMIT = pltpu.CompilerParams(vmem_limit_bytes=16 * 2**20)
SMEM = pltpu.MemorySpace.SMEM
VMEM = pltpu.MemorySpace.VMEM


def dot(a, b, dims=((1,), (0,))):
    return lax.dot_general(a, b, (dims, ((), ())), preferred_element_type=jnp.float32)


def where_1(cond):
    return jnp.where(cond, 1.0, 0.0).astype(jnp.bfloat16)


def count_kernel(mask_ref, count_ref):
    total = jnp.sum(jnp.sum(mask_ref[...], axis=0, keepdims=True), axis=1, keepdims=True)
    count_ref[...] = jnp.broadcast_to(total, (SHARDS, LANES))


def index_kernel(mask_ref, start_ref, index_ref):
    marked = mask_ref[...]
    ones = marked.astype(jnp.float32).astype(jnp.bfloat16)
    row = lax.broadcasted_iota(jnp.int32, (LANES, LANES), 0)
    lane = lax.broadcasted_iota(jnp.int32, (LANES, LANES), 1)
    full = jnp.ones((LANES, LANES), jnp.bfloat16)

    inclusive = dot(ones, where_1(row <= lane)).astype(jnp.int32)
    in_row = dot(ones, full)
    start = dot(where_1(row > lane), in_row.astype(jnp.bfloat16)).astype(jnp.int32)
    in_row_t = dot(jnp.ones((8, LANES), jnp.bfloat16), ones, ((1,), (1,)))
    start_ref[...] = dot(in_row_t.astype(jnp.bfloat16), where_1(row < lane)).astype(jnp.int32)

    moves = lane - inclusive + 1
    code = jnp.where(marked == 1, moves * 256 + lane, 0)
    for bit in range(7):
        moved = pltpu.roll(code, LANES - (1 << bit), 1)
        take = ((moved >> (8 + bit)) & 1) == 1
        leave = ((code >> (8 + bit)) & 1) == 1
        code = jnp.where(take, moved, jnp.where(leave, 0, code))
    first = start & (LANES - 1)
    nth = (lane - first) & (LANES - 1)
    source = jnp.take_along_axis(
        code & (LANES - 1), nth, axis=1, mode="promise_in_bounds"
    )
    valid = nth < in_row.astype(jnp.int32)
    here = jnp.where(valid, jnp.where(lane >= first, 256, 512), 0)
    index_ref[...] = source + here


def view_kernel(rot, trans, focal, means, scales, quats, grad, seen, out_ref, scr):
    width = 23

    def group(g, carry):
        for j in range(8):
            col = pl.ds(pl.multiple_of(g * 1024 + j * LANES, LANES), LANES)
            base = j * width
            scr[base : base + 3, :] = means[:, col]
            scr[base + 3 : base + 6, :] = scales[:, col]
            scr[base + 6 : base + 10, :] = quats[:, col]
            for v in range(VIEWS_DEV):
                scr[base + 10 + 2 * v : base + 12 + 2 * v, :] = grad[v, :, col]
            scr[base + 18 : base + 22, :] = seen[:, col].astype(jnp.float32)

        def comp(r):
            return scr[pl.ds(r, 8, stride=width), :]

        m = [comp(i) for i in range(3)]
        sc = [comp(3 + i) for i in range(3)]
        q = [comp(6 + i) for i in range(4)]
        norm = q[0] * q[0] + q[1] * q[1] + q[2] * q[2] + q[3] * q[3]
        inv = 1.0 / jnp.sqrt(norm + 0.25)
        w, x, y, z = (c * inv for c in q)
        rq = [
            [1 - 2 * (y * y + z * z), 2 * (x * y - w * z), 2 * (x * z + w * y)],
            [2 * (x * y + w * z), 1 - 2 * (x * x + z * z), 2 * (y * z - w * x)],
            [2 * (x * z - w * y), 2 * (y * z + w * x), 1 - 2 * (x * x + y * y)],
        ]
        factor = [[rq[i][j] * sc[j] for j in range(3)] for i in range(3)]
        gmax = jnp.zeros((8, LANES), jnp.float32)
        lmax = jnp.zeros((8, LANES), jnp.float32)
        for v in range(VIEWS_DEV):
            r = [[rot[i, v, j] for j in range(3)] for i in range(3)]
            f = focal[0, v]
            p = [r[i][0] * m[0] + r[i][1] * m[1] + r[i][2] * m[2] + trans[v, i] for i in range(3)]
            over = 1.0 / jnp.maximum(p[2], 1.0)
            j00 = f * over
            j02 = -(j00 * p[0]) * over
            j12 = -(j00 * p[1]) * over
            first = [j00 * r[0][j] + j02 * r[2][j] for j in range(3)]
            second = [j00 * r[1][j] + j12 * r[2][j] for j in range(3)]
            pr = [sum(first[j] * factor[j][k] for j in range(3)) for k in range(3)]
            qr = [sum(second[j] * factor[j][k] for j in range(3)) for k in range(3)]
            a = pr[0] * pr[0] + pr[1] * pr[1] + pr[2] * pr[2] + 0.3
            c = qr[0] * qr[0] + qr[1] * qr[1] + qr[2] * qr[2] + 0.3
            b = pr[0] * qr[0] + pr[1] * qr[1] + pr[2] * qr[2]
            half = 0.5 * (a - c)
            lam = 0.5 * (a + c) + jnp.sqrt(half * half + b * b + 0.01)
            vis = comp(18 + v)
            g0 = comp(10 + 2 * v)
            g1 = comp(11 + 2 * v)
            gmax = jnp.maximum(gmax, (g0 * g0 + g1 * g1) * vis)
            lmax = jnp.maximum(lmax, lam * vis)
        rows = pl.ds(pl.multiple_of(g * 8, 8), 8)
        out_ref[0, rows, :] = gmax
        out_ref[1, rows, :] = lmax
        return carry

    lax.fori_loop(0, means.shape[1] // 1024, group, 0)


def fill_kernel(
    where, counts, start, index, means, scales, quats, low, high,
    out_ref, pick_ref, table, rows
):
    view = where[0]

    @pl.when(view == 0)
    def _():
        rows[0:3, :] = means[...]
        rows[3:6, :] = scales[...]
        rows[6:8, :] = quats[0:2, :]

    @pl.when(view == 1)
    def _():
        rows[0:2, :] = quats[2:4, :]

    @pl.when(view > 1)
    def _():
        rows[0:2, :] = low[6:8, :]

    @pl.when((view > 0) & (view < 7))
    def _():
        rows[2:8, :] = high[0:6, :]

    @pl.when(view == 7)
    def _():
        rows[2:3, :] = high[0:1, :]
        rows[3:8, :] = jnp.zeros((5, G_DEV), jnp.float32)

    zero = jnp.zeros((8, LANES), jnp.float32)
    for i in range(BLOCKS):
        out_ref[i] = zero

    mine = where[1]
    total = offset = used = jnp.int32(0)
    for s in range(SHARDS):
        offset = jnp.where(s == mine, used, offset)
        local = (mine - used) & (SHARDS - 1)
        first = (used + local) >> 5
        for w in range(PER):
            table[BLOCKS + s * PER + w] = first + w
        count = counts[s, 0]
        total = total + count
        used = used + ((count + LANES - 1) >> 7)
    table[2 * BLOCKS + 1] = total
    pick = jnp.int32(0)
    for cap in CAPS[:-1]:
        pick = pick + jnp.where(used > cap * SHARDS, 1, 0)
    pick_ref[0] = pick
    table[2 * BLOCKS] = view

    def place_of(block):
        return ((offset + block) & (SHARDS - 1)) * PER + (block >> 5)

    def some(i, carry):
        for j in range(32):
            b = i * 32 + j
            block = start[0, b] >> 7
            here = place_of(block)
            after = place_of(jnp.minimum(block + 1, BLOCKS - 1))
            table[b] = here + (after << 8)
            code = jnp.broadcast_to(index[pl.ds(b, 1), :], (8, LANES))
            tile = rows[:, pl.ds(pl.multiple_of(b * LANES, LANES), LANES)]
            packed = jnp.take_along_axis(
                tile, code & (LANES - 1), axis=1, mode="promise_in_bounds"
            )
            pltpu.store(out_ref.at[here], packed, mask=(code & 256) != 0)
            pltpu.store(out_ref.at[after], packed, mask=(code & 512) != 0)
        return carry

    lax.fori_loop(0, BLOCKS // 32, some, 0)


def top_of(squares, k, at):
    a, b, c, d = (sq[k, at, :] for sq in squares)
    return jnp.maximum(jnp.maximum(a, b), jnp.maximum(c, d))


def add_kernel(table, index, sq0, sq1, sq2, sq3, filled, out_ref, top_ref, pairs):
    for g in range(BLOCKS // 8):
        at = slice(8 * g, 8 * g + 8)
        for k in range(2):
            top_ref[k, at, :] = top_of((sq0, sq1, sq2, sq3), k, at)

    @pl.when(table[2 * BLOCKS] == 7)
    def _():
        for g in range(BLOCKS // 8):
            at = slice(8 * g, 8 * g + 8)
            lanes = index[at, :] & (LANES - 1)
            for k in range(2):
                root = jnp.sqrt(top_ref[k, at, :])
                pairs[pl.ds(16 * g + k, 8, stride=2), :] = jnp.take_along_axis(
                    root if k == 0 else 3.0 * root, lanes, axis=1, mode="promise_in_bounds"
                )
        for b in range(BLOCKS):
            both = table[b]
            code = jnp.broadcast_to(index[b : b + 1, :], (2, LANES))
            two = pairs[2 * b : 2 * b + 2, :]
            pltpu.store(out_ref.at[both & 255, 3:5, :], two, mask=(code & 256) != 0)
            pltpu.store(out_ref.at[both >> 8, 3:5, :], two, mask=(code & 512) != 0)


def place_kernel(table, arrived, out_ref, slots):
    cap = out_ref.shape[1]
    zero = jnp.zeros((8, LANES), jnp.float32)
    for i in range(cap):
        slots[i] = zero
    for i in range(BLOCKS):
        slots[jnp.minimum(table[BLOCKS + i], cap)] = arrived[i]
    for i in range(cap):
        tile = slots[i]
        for x in range(4):
            out_ref[x, i] = tile


def row_copy(buf, out_ref, sems, r, columns):
    rows = min(8, ROWS - 8 * r)
    return pltpu.make_async_copy(
        buf.at[r, 0:rows, columns], out_ref.at[8 * r : 8 * r + rows, columns], sems.at[r]
    )


def own_kernel(table, own, out_ref, total_ref, buf, zeros, sems):
    cap = own.shape[1]
    core = table[2 * BLOCKS] & 1
    total_ref[0] = table[2 * BLOCKS + 1]

    def clear(r):
        rows = min(8, ROWS - 8 * r)
        return pltpu.make_async_copy(
            zeros.at[0:rows, :],
            out_ref.at[8 * r : 8 * r + rows, cap * LANES : G_DEV],
            sems.at[8 + r],
        )

    if cap < BLOCKS:
        for i in range(BLOCKS - cap):
            zeros[:, i * LANES : (i + 1) * LANES] = jnp.zeros((8, LANES), jnp.float32)
        for r in range(8):
            clear(r).start()
    for half in range(2):

        @pl.when(core == half)
        def _():
            for r in range(half, 8, 2):
                for i in range(cap):
                    buf[r, :, i * LANES : (i + 1) * LANES] = own[r // 2, i]
                row_copy(buf, out_ref, sems, r, slice(0, cap * LANES)).start()

    for half in range(2):

        @pl.when(core == half)
        def _():
            for r in range(half, 8, 2):
                row_copy(buf, out_ref, sems, r, slice(0, cap * LANES)).wait()

    if cap < BLOCKS:
        for r in range(8):
            clear(r).wait()


def other_kernel(
    table, other, top, mate, begun, out_ref, peak_ref, buf, pairs, peaks, sems
):
    cap = other.shape[1]
    core = table[2 * BLOCKS] & 1
    for half in range(2):

        @pl.when(core == half)
        def _():
            for r in range(1 - half, 8, 2):
                for i in range(cap):
                    buf[r, :, i * LANES : (i + 1) * LANES] = other[r // 2, i]
                row_copy(buf, out_ref, sems, r, slice(0, cap * LANES)).start()

    for g in range(BLOCKS // 8):
        at = slice(8 * g, 8 * g + 8)
        norm = jnp.sqrt(jnp.maximum(top[0, at, :], mate[0, at, :]))
        radius = 3.0 * jnp.sqrt(jnp.maximum(top[1, at, :], mate[1, at, :]))
        pairs[pl.ds(16 * g, 8, stride=2), :] = norm
        pairs[pl.ds(16 * g + 1, 8, stride=2), :] = radius
    for b in range(BLOCKS):
        peaks[:, b * LANES : (b + 1) * LANES] = pairs[2 * b : 2 * b + 2, :]
    peak_copy = pltpu.make_async_copy(peaks, peak_ref, sems.at[8])
    peak_copy.start()

    for half in range(2):

        @pl.when(core == half)
        def _():
            for r in range(1 - half, 8, 2):
                row_copy(buf, out_ref, sems, r, slice(0, cap * LANES)).wait()

    peak_copy.wait()


def smem():
    return pl.BlockSpec(memory_space=SMEM)


def vmem():
    return pl.BlockSpec(memory_space=VMEM)


def body(means, scales, quats, attrs, grad_screen, visible, clone_mask, rotation, shift, focal):
    f32, i32 = jnp.float32, jnp.int32
    view = lax.axis_index("view")
    where = jnp.stack([view, lax.axis_index("gauss")]).astype(i32)

    def whole(*shape):
        return pl.BlockSpec(shape, lambda i, w: (0,) * len(shape))

    mask = clone_mask.reshape(BLOCKS, LANES)
    rotation, focal = rotation.transpose(1, 0, 2), focal.reshape(1, VIEWS_DEV)
    mask, means, scales, quats, attrs, grad_screen, visible, rotation, shift, focal = (
        pltpu.with_memory_space_constraint(x, pltpu.MemorySpace.HBM)
        for x in (
            mask, means, scales, quats, attrs, grad_screen, visible, rotation, shift, focal
        )
    )
    count = pl.pallas_call(
        count_kernel,
        in_specs=[vmem()],
        out_specs=vmem(),
        out_shape=VMEM((SHARDS, LANES), i32),
        compiler_params=LIMIT,
        name="count",
    )(mask)
    counts = lax.all_to_all(count, "gauss", 0, 0, tiled=True)

    squares = pl.pallas_call(
        view_kernel,
        in_specs=[smem()] * 3 + [vmem()] * 5,
        out_specs=vmem(),
        out_shape=VMEM((2, BLOCKS, LANES), f32),
        scratch_shapes=[pltpu.VMEM((216, LANES), f32)],
        compiler_params=LIMIT,
        name="views",
    )(rotation, shift, focal, means, scales, quats, grad_screen, visible)
    other = lax.ppermute(squares, "view", [(v, v ^ 1) for v in range(8)])
    squares = [jnp.maximum(squares, other)]
    for k in (1, 2, 3):
        pairs = [(v, (v + 2 * k) % 8) for v in (1, 3, 5, 7)]
        squares.append(lax.ppermute(squares[0], "view", pairs))

    start, index = pl.pallas_call(
        index_kernel,
        in_specs=[vmem()],
        out_specs=[vmem()] * 2,
        out_shape=[
            VMEM((8, LANES), i32),
            VMEM((BLOCKS, LANES), i32),
        ],
        compiler_params=LIMIT,
        name="index",
    )(mask)
    filled, branch, table = pl.pallas_call(
        fill_kernel,
        grid_spec=pltpu.PrefetchScalarGridSpec(
            num_scalar_prefetch=1,
            grid=(1,),
            in_specs=[
                smem(),
                smem(),
                whole(BLOCKS, LANES),
                whole(3, G_DEV),
                whole(3, G_DEV),
                whole(4, G_DEV),
                pl.BlockSpec((8, G_DEV), lambda i, w: (jnp.maximum(w[0] - 2, 0), 0)),
                pl.BlockSpec((8, G_DEV), lambda i, w: (jnp.maximum(w[0] - 1, 0), 0)),
            ],
            out_specs=[whole(BLOCKS, 8, LANES), smem(), smem()],
            scratch_shapes=[pltpu.VMEM((8, G_DEV), f32)],
        ),
        out_shape=[
            VMEM((BLOCKS, 8, LANES), f32),
            SMEM((1,), i32),
            SMEM((3 * BLOCKS,), i32),
        ],
        compiler_params=LIMIT,
        name="fill",
    )(where, counts, start, index, means, scales, quats, attrs, attrs)
    outgoing, top = pl.pallas_call(
        add_kernel,
        in_specs=[smem()] + [vmem()] * 6,
        out_specs=[vmem()] * 2,
        out_shape=[VMEM((BLOCKS, 8, LANES), f32), VMEM((2, BLOCKS, LANES), f32)],
        input_output_aliases={6: 0},
        scratch_shapes=[pltpu.VMEM((2 * BLOCKS + 32, LANES), f32)],
        compiler_params=LIMIT,
        name="add",
    )(table, index, *squares, filled)

    def gather(cap):
        def go(table, outgoing, top):
            arrived = lax.all_to_all(
                outgoing.reshape(SHARDS, PER, 8, LANES), "gauss", 0, 0, tiled=True
            ).reshape(BLOCKS, 8, LANES)
            piece = pl.pallas_call(
                place_kernel,
                in_specs=[smem(), vmem()],
                out_specs=vmem(),
                out_shape=VMEM((4, cap, 8, LANES), f32),
                scratch_shapes=[pltpu.VMEM((cap + 1, 8, LANES), f32)],
                compiler_params=LIMIT,
                name="place",
            )(table, arrived)
            cores = [[0, 2, 4, 6], [1, 3, 5, 7]]
            own = lax.all_to_all(piece, "view", 0, 0, axis_index_groups=cores, tiled=True)
            mate = lax.ppermute(top, "view", [(1, 0), (3, 2), (5, 4), (7, 6)])
            own, mate = lax.optimization_barrier((own, mate))
            other = lax.ppermute(own, "view", [(v, v ^ 1) for v in range(8)])
            begun, total = pl.pallas_call(
                own_kernel,
                in_specs=[smem(), vmem()],
                out_specs=[pl.BlockSpec(memory_space=pl.ANY), smem()],
                out_shape=[
                    jax.ShapeDtypeStruct((ROWS, G_DEV), f32),
                    pltpu.MemorySpace.HBM((1,), i32),
                ],
                scratch_shapes=[
                    pltpu.VMEM((8, 8, cap * LANES), f32),
                    pltpu.VMEM((8, max(BLOCKS - cap, 1) * LANES), f32),
                    pltpu.SemaphoreType.DMA((16,)),
                ],
                compiler_params=LIMIT,
                name="own",
            )(table, own)
            clones, peak = pl.pallas_call(
                other_kernel,
                in_specs=[smem(), vmem(), vmem(), vmem(), pl.BlockSpec(memory_space=pl.ANY)],
                out_specs=[pl.BlockSpec(memory_space=pl.ANY)] * 2,
                out_shape=[
                    jax.ShapeDtypeStruct((ROWS, G_DEV), f32),
                    pltpu.MemorySpace.HBM((2, G_DEV), f32),
                ],
                input_output_aliases={4: 0},
                scratch_shapes=[
                    pltpu.VMEM((8, 8, cap * LANES), f32),
                    pltpu.VMEM((2 * BLOCKS + 32, LANES), f32),
                    pltpu.VMEM((2, G_DEV), f32),
                    pltpu.SemaphoreType.DMA((9,)),
                ],
                compiler_params=LIMIT,
                name="other",
            )(table, other, top, mate, begun)
            return peak, clones, total

        return go

    peak, clones, total = lax.switch(
        branch[0], [gather(cap) for cap in CAPS], table, outgoing, top
    )
    return (peak, clones, total[0])


def solution(mesh):
    return jax.shard_map(
        body,
        mesh=mesh,
        in_specs=(
            P(None, "gauss"),
            P(None, "gauss"),
            P(None, "gauss"),
            P(None, "gauss"),
            P("view", None, "gauss"),
            P("view", "gauss"),
            P("gauss"),
            P("view", None, None),
            P("view", None),
            P("view"),
        ),
        out_specs=(P(None, "gauss"), P(None, "gauss"), P()),
        check_vma=False,
    )
```
